32 devices in a mesh: tile: 8 (over z, y), depth: 4 (over x, core).
Axes of the slice: x: 2, y: 2, z: 4, core: 2. Of those that a mesh axis runs over, the one named last changes fastest.
Arguments:
- positions: float32 [3, 16384], P(None, 'tile'), may hold values from -4 to 4
- log_scales: float32 [3, 16384], P(None, 'tile'), may hold values from -2 to 0
- opacity_logits: float32 [1, 16384], P(None, 'tile'), may hold values from -3 to 1.5
- colors: float32 [3, 16384], P(None, 'tile'), may hold values from 0 to 1
- first_moment: float32 [10, 16384], P(None, 'tile'), may hold values from -3 to 3
- second_moment: float32 [10, 16384], P(None, 'tile'), may hold values from 0.01 to 1
- cameras: float32 [4, 2, 4], replicated, may hold values from -6.4 to 6.4
- background: float32 [3], replicated, may hold values from 0 to 1
- target: float32 [32, 3, 1024], P('tile'), may hold values from 0 to 1
- tile_view: int32 [32], P('tile'), may hold values from 0 to 3
- tile_length: int32 [32], P('tile'), may hold values from 128 to 512
- list_owner: int32 [4, 32, 128, 1], P('depth', 'tile'), may hold values from 0 to 7; in each aligned block of 512 rows (0 to 511, 512 to 1023, ..., all dimensions but the last counted through in order) at most 160 rows name the same one
- list_row: int32 [4, 32, 128], P('depth', 'tile'), may hold values from 0 to 2047
Outputs:
- image: float32 [32, 3, 1024], P('tile')
- new_params: float32 [10, 16384], P(None, 'tile')
- new_first: float32 [10, 16384], P(None, 'tile')
- new_second: float32 [10, 16384], P(None, 'tile')
The draws below stay inside these ranges and needn't reach their ends.
Inputs may be any that keep to these rules, and one draw needn't show every extreme that they name: `list_owner`: within the entries of one device's block (one depth slab of the tiles of one tile index), no owner is named more than 160 times, a bound that some block reaches.
All inputs are finite; a program needn't handle non-finite values.
Results may differ from the reference program's by a relative error of at most 0.00008.
Values sent between devices are 32-bit elements; how exact they have to be, the bound alone decides.
A program may use at most 64 MiB of HBM per device.

```python
import math
import jax
import jax.numpy as jnp
import numpy as np
from jax import lax

TILE_SIDE = 32
PIX = 1024
LIST = 512
VIEWS = 4
TILES_DEV = 4
G_DEV = 2048
TILES = 32
SPLATS = 16384
SLAB = 128
CAP = 160
N_TILE = 8
N_DEPTH = 4


def with_ends(drawn, rng, smallest, top_value):
    spot = [jax.random.randint(jax.random.fold_in(rng, axis), (), 0, length) for axis, length in enumerate(drawn.shape)]
    main_axis = drawn.shape.index(max(drawn.shape))
    neighbour = spot[:main_axis] + [(spot[main_axis] + 1) % drawn.shape[main_axis]] + spot[main_axis + 1:]
    return drawn.at[tuple(spot)].set(smallest).at[tuple(neighbour)].set(top_value)


def shard_levels(rng, extent, shards, least, top_value):
    level = 1.0
    for dim, blocks in shards:
        draws = jax.random.uniform(jax.random.fold_in(jax.random.fold_in(rng, 6), dim), (blocks,), jnp.float32, least / len(shards), top_value / len(shards))
        level = level * jnp.repeat(jnp.exp(draws), extent[dim] // blocks).reshape((-1,) + (1,) * (len(extent) - 1 - dim))
    return level


def deal_out(key, own, number, rows, count, top, limit, slope):
    order = jax.random.permutation(key, count)
    crowded, usual = portions_of(count, rows * top, limit, slope, True), portions_of(count, rows * top, limit, slope, False)
    places = jnp.arange(count)

    def named(tallies, turn):
        used = int((tallies > 0).sum())
        fixed = max(1, used // 4)
        passed = fixed + (places - fixed + turn * (used - fixed)) % max(1, count - fixed)
        return jnp.zeros((count,), jnp.int32).at[order[jnp.where(places < fixed, places, passed)]].set(jnp.asarray(tallies, jnp.int32))

    tallies = jnp.where(number % 4 == 0, named(crowded, number // 4), named(usual, number - number // 4 - 1))
    mixed = jax.random.permutation(jax.random.fold_in(own, 3), count)
    donor, sink = mixed[0:count // 2 * 2:2], mixed[1:count // 2 * 2:2]
    margin = jnp.minimum(tallies[donor] - 1, limit - tallies[sink]) // 2
    margin = jnp.where((donor == order[0]) | (sink == order[0]) | (tallies[sink] == 0), 0, jnp.maximum(margin, 0))
    passed = jax.random.randint(jax.random.fold_in(own, 4), (count // 2,), 0, 1 << 20) % (margin + 1)
    tallies = tallies.at[donor].add(-passed).at[sink].add(passed)
    labels = jnp.searchsorted(jnp.cumsum(tallies), jnp.arange(rows * top), side="right").astype(jnp.int32)
    table = labels.reshape(top, rows).T
    table = table[jax.random.permutation(jax.random.fold_in(own, 1), rows)]
    turn = jax.random.randint(jax.random.fold_in(own, 2), (rows, 1), 0, top)
    return jnp.take_along_axis(table, (jnp.arange(top)[None, :] + turn) % top, axis=1)


def portions_of(number_of, total, bound, lean, full):
    loads = [(1 << 20) // math.isqrt(standing ** lean) + 1 for standing in range(1, number_of + 1)]
    largest = bound if full else min(bound, max(-(-total // number_of), total * loads[0] // sum(loads)))
    least = 1 if total - largest >= number_of - 1 else 0
    given, surplus = [largest] + [least] * (number_of - 1), total - largest - least * (number_of - 1)
    while surplus > 0:
        movable = [i for i in range(1, number_of) if given[i] < largest] or [i for i in range(1, number_of) if given[i] < bound]
        whole, budget = sum([loads[i] for i in movable]), surplus
        for i in movable:
            extra = min(bound - given[i], max(1, budget * loads[i] // whole), surplus)
            given[i] = given[i] + extra
            surplus = surplus - extra
    return np.array(given)


def normal_values(key, shape, scale, most, split=(), kind=jnp.bfloat16):
    values = scale * jax.random.normal(key, shape, jnp.float32)
    if split:
        values = values * shard_levels(key, shape, split, -0.22, 0.18)
    return jnp.clip(values, -most, most).astype(kind)


def setup_inputs(seed: int = 0) -> dict:
    seeds = jax.random.split(jax.random.key(seed), 14)
    positions = normal_values(seeds[0], (3, SPLATS), 1.0, 4.0, ((1, 8),), jnp.float32)
    log_scales = jnp.clip(-2.0 + 2.0 * jax.random.uniform(seeds[1], (3, SPLATS), jnp.float32) ** shard_levels(seeds[1], (3, SPLATS), ((1, 8),), -0.2, 0.2), -2.0, 0.0)
    opacity_logits = jnp.clip(-3.0 + 4.5 * jax.random.uniform(seeds[2], (1, SPLATS), jnp.float32) ** shard_levels(seeds[2], (1, SPLATS), ((1, 8),), -0.2, 0.2), -3.0, 1.5)
    colors = jnp.clip(1.0 * jax.random.uniform(seeds[3], (3, SPLATS), jnp.float32) ** shard_levels(seeds[3], (3, SPLATS), ((1, 8),), -0.2, 0.2), 0.0, 1.0)
    first_moment = normal_values(seeds[4], (10, SPLATS), 0.5, 3.0, ((1, 8),), jnp.float32)
    second_moment = jnp.clip(jnp.exp(math.log(1.0) - 4.6051702 * jax.random.uniform(seeds[5], (10, SPLATS), jnp.float32) ** shard_levels(seeds[5], (10, SPLATS), ((1, 8),), -0.2, 0.2)), 0.01, 1.0)
    cameras = jnp.clip(jax.random.uniform(seeds[6], (VIEWS, 2, 4), jnp.float32, -6.4, 6.4), -6.4, 6.4)
    background = jnp.clip(jax.random.uniform(seeds[7], (3,), jnp.float32, 0.0, 1.0), 0.0, 1.0)
    target = jnp.clip(1.0 * jax.random.uniform(seeds[8], (TILES, 3, PIX), jnp.float32) ** shard_levels(seeds[8], (TILES, 3, PIX), ((0, 8),), -0.2, 0.2), 0.0, 1.0)
    tile_view = with_ends(jax.random.randint(seeds[9], (TILES,), 0, VIEWS), jax.random.fold_in(seeds[9], 1), 0, VIEWS - 1).astype(jnp.int32)
    tile_length = with_ends(jax.random.randint(seeds[10], (TILES,), LIST // 4, LIST + 1), jax.random.fold_in(seeds[10], 1), LIST // 4, LIST).astype(jnp.int32)
    list_owner_keys = jax.random.split(jax.random.fold_in(seeds[11], 1), N_DEPTH * TILES * SLAB // (TILES_DEV * SLAB))
    list_owner_turns = jax.random.permutation(jax.random.fold_in(seeds[11], 3), N_DEPTH * TILES * SLAB // (TILES_DEV * SLAB))
    list_owner = jax.vmap(lambda own, number: deal_out(jax.random.fold_in(seeds[11], 2), own, number, TILES_DEV * SLAB, N_TILE, 1, CAP, 2))(list_owner_keys, list_owner_turns).reshape((N_DEPTH, TILES, SLAB, 1))
    list_row = with_ends(jax.random.randint(seeds[12], (N_DEPTH, TILES, SLAB), 0, G_DEV), jax.random.fold_in(seeds[12], 1), 0, G_DEV - 1).astype(jnp.int32)
    return dict(positions=positions, log_scales=log_scales, opacity_logits=opacity_logits, colors=colors, first_moment=first_moment, second_moment=second_moment, cameras=cameras, background=background, target=target, tile_view=tile_view, tile_length=tile_length, list_owner=list_owner, list_row=list_row)


def project(params, cams):
    position = params[0:3]
    variance = jnp.exp(2.0 * params[3:6])
    first_row = cams[:, 0, 0:3].T
    second_row = cams[:, 1, 0:3].T
    center_x = lax.optimization_barrier(jnp.sum(first_row * position, axis=0)) + cams[:, 0, 3] + 0.5 * TILE_SIDE
    center_y = lax.optimization_barrier(jnp.sum(second_row * position, axis=0)) + cams[:, 1, 3] + 0.5 * TILE_SIDE
    cov_xx = lax.optimization_barrier(jnp.sum(first_row * first_row * variance, axis=0)) + 0.3
    cov_xy = lax.optimization_barrier(jnp.sum(first_row * second_row * variance, axis=0))
    cov_yy = lax.optimization_barrier(jnp.sum(second_row * second_row * variance, axis=0)) + 0.3
    determinant = cov_xx * cov_yy - cov_xy * cov_xy
    return jnp.stack([center_x, center_y, cov_yy / determinant, -cov_xy / determinant, cov_xx / determinant, jax.nn.sigmoid(params[6]), params[7], params[8], params[9]])

def render_tile(screen, alive, background):
    pixel = jnp.arange(PIX, dtype=jnp.int32)
    pixel_x = (pixel % TILE_SIDE).astype(jnp.float32) + 0.5
    pixel_y = (pixel // TILE_SIDE).astype(jnp.float32) + 0.5
    offset_x = pixel_x[:, None] - screen[0][None, :]
    offset_y = pixel_y[:, None] - screen[1][None, :]
    quadric = screen[2][None, :] * offset_x * offset_x + 2.0 * screen[3][None, :] * offset_x * offset_y + screen[4][None, :] * offset_y * offset_y
    alpha = screen[5][None, :] * jnp.exp(-0.5 * quadric) * alive[None, :]
    leak = jnp.log1p(-alpha)
    before = jnp.cumsum(leak, axis=1) - leak
    weight = alpha * jnp.exp(before)
    color = jnp.einsum('ck,pk->cp', screen[6:9], weight, precision=lax.Precision.HIGHEST)
    return color + jnp.exp(lax.optimization_barrier(jnp.sum(leak, axis=1)))[None, :] * background[:, None]

def reference(positions, log_scales, opacity_logits, colors, first_moment, second_moment, cameras, background, target, tile_view, tile_length, list_owner, list_row):
    params = jnp.concatenate([positions, log_scales, opacity_logits, colors], axis=0)
    ident = (list_owner[..., 0] * G_DEV + list_row).astype(jnp.int32)
    ident = jnp.transpose(ident, (1, 0, 2)).reshape(TILES, LIST)
    live = (jnp.arange(LIST, dtype=jnp.int32)[None, :] < tile_length[:, None]).astype(jnp.float32)

    def render(values):

        def single(args):
            names, view, alive = args
            cams = jnp.broadcast_to(cameras[view], (LIST, 2, 4))
            screen = project(values[:, names], cams)
            return render_tile(screen, alive, background)
        return lax.map(jax.checkpoint(single), (ident, tile_view, live))
    image, pullback = jax.vjp(render, params)
    gradient, = pullback(image - target)
    new_first = 0.9 * first_moment + 0.1 * gradient
    new_second = 0.999 * second_moment + 0.001 * gradient * gradient
    corrected = new_first / (1.0 - 0.9 ** 10) / (jnp.sqrt(new_second / (1.0 - 0.999 ** 10)) + 1e-08)
    new_params = params - 0.05 * corrected
    return (image, new_params, new_first, new_second)
```

```python
import functools

import jax
import jax.numpy as jnp
from jax import lax
from jax.experimental import pallas as pl
from jax.experimental.pallas import tpu as pltpu
from jax.sharding import PartitionSpec as P

TILE_SIDE = 32
LANES = 128
MESH = pl.DeviceIdType.MESH
F32 = jnp.float32
BF16 = jnp.bfloat16


def greet(peers):
    barrier = pltpu.get_barrier_semaphore()
    for peer in peers:
        pl.semaphore_signal(barrier, inc=1, device_id=peer, device_id_type=MESH)
    pl.semaphore_wait(barrier, len(peers))


def remote(source, target, send, receive, peer):
    return pltpu.make_async_remote_copy(
        src_ref=source, dst_ref=target, send_sem=send, recv_sem=receive,
        device_id=peer, device_id_type=MESH,
    )


def split3(x):
    high = x.astype(BF16)
    rest = x - high.astype(F32)
    middle = rest.astype(BF16)
    low = (rest - middle.astype(F32)).astype(BF16)
    return high, middle, low


def flip(index, step, size):
    out, bit = 0, 1
    while bit < size:
        mine = lax.rem(lax.div(index, bit), 2)
        if isinstance(step, int):
            out = out + bit * (1 - mine if (step // bit) % 2 else mine)
        else:
            out = out + bit * lax.rem(mine + lax.rem(lax.div(step, bit), 2), 2)
        bit *= 2
    return out


def step_kernel(
    tiles, depths,
    owner_in, row_in, place_in, scale_in, logit_in, color_in, first_in, second_in,
    target_in, view_in, length_in, cam_in, back_in,
    picture_ref, new_param_ref, new_first_ref, new_second_ref,
    owner_ref, row_ref, place_ref, scale_ref, logit_ref, color_ref, first_ref, second_ref,
    target_ref, view_ref, length_ref, cam_ref, back_ref, loads,
    named_ref, lists_ref, param_ref, high_ref, low_ref, answers, got,
    ask_send, ask_recv, send, receive,
    alphas, weights, misses, carries, columns, sums, grad_ref, image_ref, images_ref,
    inbox, partial, half_in, half_sum, pieces, whole_out,
    grad_send, grad_recv, image_send, image_recv, pair_send, pair_recv, cut_send, cut_recv,
    all_send, all_recv,
):
    lines = param_ref.shape[0]
    highs = lines // 10
    slabs, _, slab = named_ref.shape
    entries = slabs * slab
    pixels = target_ref.shape[2]
    splats = highs * LANES
    me_t, me_d = lax.axis_index("tile"), lax.axis_index("depth")
    small = tiles <= 8
    depth_of = [me_d] + [flip(me_d, b, depths) for b in range(1, depths)]
    tile_of = [me_t] + [flip(me_t, a, tiles) for a in range(1, tiles)] if small else None
    steps = [(a, b) for a in range(tiles - 1, -1, -1) for b in range(depths) if a or b]

    def tile_at(step):
        return tile_of[step] if small else flip(me_t, step, tiles)

    def to(a, b):
        return {"tile": tile_at(a), "depth": depth_of[b]}

    def across(step):
        return {"tile": tile_at(step)}

    def along(step):
        return {"depth": depth_of[step]}

    def each_tile(function):
        if small:
            for step in range(1, tiles):
                function(step)
        else:
            def one(step, carry):
                function(step)
                return carry

            lax.fori_loop(1, tiles, one, 0)

    barrier = pltpu.get_barrier_semaphore()
    for a, b in steps:
        pl.semaphore_signal(barrier, inc=1, device_id=to(a, b), device_id_type=MESH)
    pairs = [
        (owner_in, owner_ref), (row_in, row_ref), (place_in, place_ref), (scale_in, scale_ref),
        (logit_in, logit_ref), (color_in, color_ref), (view_in, view_ref), (length_in, length_ref),
        (cam_in, cam_ref), (back_in, back_ref), (target_in, target_ref),
        (first_in, first_ref), (second_in, second_ref),
    ]
    copies = [
        pltpu.make_async_copy(source, target, loads.at[i])
        for i, (source, target) in enumerate(pairs)
    ]
    for copy in copies:
        copy.start()
    for copy in copies[:2]:
        copy.wait()
    for q in range(slabs):
        named_ref[q] = owner_ref[q] * splats + row_ref[q : q + 1, :]
    pl.semaphore_wait(barrier, len(steps))

    def asked(a, b):
        return remote(
            named_ref.at[depth_of[b]], lists_ref.at[me_t, me_d],
            ask_send.at[a, b], ask_recv.at[a, b], to(a, b),
        )

    for a, b in steps:
        asked(a, b).start()
    lists_ref[me_t, me_d] = named_ref[me_d]
    for copy in copies[2:6]:
        copy.wait()
    param = 0
    for ref in (place_ref, scale_ref, logit_ref, color_ref):
        for k in range(ref.shape[0]):
            for h in range(highs):
                line = param * highs + h
                param_ref[line : line + 1, :] = ref[k : k + 1, h * LANES : (h + 1) * LANES]
            param += 1
    high, middle, low = split3(param_ref[...])
    high_ref[...] = jnp.concatenate([high, middle], axis=1)
    low_ref[...] = low
    low_iota = lax.broadcasted_iota(jnp.int32, (LANES, entries), 0)
    high_iota = lax.broadcasted_iota(jnp.int32, (highs, entries), 0) + me_t * highs

    def entry_names(slot):
        names = jnp.concatenate([lists_ref[slot, d] for d in range(slabs)], axis=1)
        onehot = jnp.where(low_iota == (names & (LANES - 1)), 1.0, 0.0).astype(BF16)
        return onehot, high_iota == (names >> 7)

    def answer(slot):
        onehot, mask = entry_names(slot)
        twice = jnp.concatenate([onehot, onehot], axis=0)
        found = jnp.dot(high_ref[...], twice, preferred_element_type=F32) + jnp.dot(
            low_ref[...], onehot, preferred_element_type=F32
        )
        return jnp.concatenate(
            [
                jnp.sum(
                    jnp.where(mask, found[p * highs : (p + 1) * highs], 0.0), axis=0, keepdims=True
                )
                for p in range(10)
            ],
            axis=0,
        )

    def put(ref, step, rows):
        for j in range(slabs):
            ref[step, j * 10 : (j + 1) * 10, :] = rows[:, j * slab : (j + 1) * slab]

    def back(step):
        return remote(
            answers.at[step], got.at[step], send.at[step], receive.at[step], across(step)
        )

    def serve(step):
        for b in range(depths):
            asked(step, b).wait_recv()
        put(answers, step, answer(tile_at(step)))
        back(step).start()

    each_tile(serve)
    for b in range(1, depths):
        asked(0, b).wait_recv()
    put(got, 0, answer(me_t))
    for a, b in steps:
        asked(a, b).wait_send()
    for copy in copies[6:]:
        copy.wait()

    def take(step):
        back(step).wait()
        got[0] += got[step]

    each_tile(take)
    found = got[0]

    chunks = pixels // LANES
    groups = entries // 8
    length = length_ref[me_d]
    view = view_ref[me_d]
    values = [
        jnp.concatenate([found[j * 10 + p : j * 10 + p + 1, :] for j in range(slabs)], axis=1)
        for p in range(10)
    ]

    first = [cam_ref[view, 0, j] for j in range(4)]
    second = [cam_ref[view, 1, j] for j in range(4)]
    variance = [jnp.exp(2.0 * values[3 + j]) for j in range(3)]
    half = 0.5 * TILE_SIDE
    center_x = first[0] * values[0] + first[1] * values[1] + first[2] * values[2] + first[3] + half
    center_y = second[0] * values[0] + second[1] * values[1] + second[2] * values[2] + second[3] + half
    cov_xx = sum(first[j] * first[j] * variance[j] for j in range(3)) + 0.3
    cov_xy = sum(first[j] * second[j] * variance[j] for j in range(3))
    cov_yy = sum(second[j] * second[j] * variance[j] for j in range(3)) + 0.3
    determinant = cov_xx * cov_yy - cov_xy * cov_xy
    conic_a = cov_yy / determinant
    conic_b = -cov_xy / determinant
    conic_c = cov_xx / determinant
    opacity = 1.0 / (1.0 + jnp.exp(-values[6]))
    place = lax.broadcasted_iota(jnp.int32, (1, entries), 1)
    shown = jnp.where(place < length, opacity, 0.0)
    rows = [center_x, center_y, -0.5 * conic_a, -conic_b, -0.5 * conic_c, shown] + values[7:10]
    table = jnp.concatenate(rows + [jnp.zeros((LANES - len(rows), entries), F32)], axis=0)
    columns[...] = table.T

    lane = lax.broadcasted_iota(jnp.int32, (8, LANES), 1)
    sub = lax.broadcasted_iota(jnp.int32, (8, LANES), 0)
    pixel_x = (lane & (TILE_SIDE - 1)).astype(F32) + 0.5
    pixel_y = (lane >> 5).astype(F32) + 0.5
    rows_chunk = LANES // TILE_SIDE
    ones = jnp.ones((8, LANES), F32)

    def spread(cols, j):
        return jnp.broadcast_to(cols[:, j : j + 1], (8, LANES))

    def forward(g, carry):
        trans, color = carry
        at = pl.ds(pl.multiple_of(g * 8, 8), 8)
        cols = columns[pl.ds(g, 8, stride=groups), :]
        cx, cy, qa, qb, qc, op, red, green, blue = [spread(cols, j) for j in range(9)]
        ex = pixel_x - cx
        ey0 = pixel_y - cy
        qaxx = qa * ex * ex
        qbx = qb * ex
        new_trans, new_color = [], []
        for c in range(chunks):
            ey = ey0 + float(c * rows_chunk)
            alpha = op * jnp.exp(qaxx + (qbx + qc * ey) * ey)
            t = trans[c]
            part = slice(c * LANES, (c + 1) * LANES)
            alphas[at, part] = alpha
            weight = alpha * t
            weights[at, part] = weight
            new_trans.append(t - weight)
            new_color.append(color[3 * c] + weight * red)
            new_color.append(color[3 * c + 1] + weight * green)
            new_color.append(color[3 * c + 2] + weight * blue)
        return new_trans, new_color

    zeros = jnp.zeros((8, LANES), F32)
    trans, color = lax.fori_loop(
        0, groups, forward, ([ones] * chunks, [zeros] * (3 * chunks)), unroll=4
    )

    chosen = lax.broadcasted_iota(jnp.int32, (slabs, LANES), 0) == me_d
    behinds = []
    for c in range(chunks):
        part = slice(c * LANES, (c + 1) * LANES)
        run = jnp.where(sub >= 1, pltpu.roll(trans[c], 1, 0), 1.0)
        for s in (1, 2, 4):
            run = run * jnp.where(sub >= s, pltpu.roll(run, s, 0), 1.0)
        carries[:, part] = run
        left = (run * trans[c])[7:8, :]
        total = 0.0
        pulled = zeros
        for k in range(3):
            lit = run * color[3 * c + k]
            shade = jnp.sum(lit, axis=0, keepdims=True) + left * back_ref[k]
            image_ref[k : k + 1, part] = shade
            miss = shade - jnp.sum(
                jnp.where(chosen, target_ref[k, :, part], 0.0), axis=0, keepdims=True
            )
            misses[k, :, part] = jnp.broadcast_to(miss, (8, LANES))
            total = total + miss * shade
            pulled = pulled + miss * lit
        ahead = jnp.where(sub >= 1, pltpu.roll(pulled, 1, 0), 0.0)
        for s in (1, 2, 4):
            ahead = ahead + jnp.where(sub >= s, pltpu.roll(ahead, s, 0), 0.0)
        behinds.append(total - ahead)

    images_ref[me_d] = image_ref[...]
    image_copies = [
        remote(image_ref, images_ref.at[me_d], image_send.at[s], image_recv.at[s], along(s))
        for s in range(1, depths)
    ]
    for copy in image_copies:
        copy.start()

    def backward(g, behind):
        at = pl.ds(pl.multiple_of(g * 8, 8), 8)
        spaced = pl.ds(g, 8, stride=groups)
        cols = columns[spaced, :]
        cx, cy, red, green, blue = [spread(cols, j) for j in (0, 1, 6, 7, 8)]
        ex = pixel_x - cx
        ey0 = pixel_y - cy
        new_behind = []
        acc = [zeros] * 6
        for c in range(chunks):
            part = slice(c * LANES, (c + 1) * LANES)
            alpha = alphas[at, part]
            weight = weights[at, part] * carries[:, part]
            m0, m1, m2 = misses[0, :, part], misses[1, :, part], misses[2, :, part]
            pull = m0 * red + m1 * green + m2 * blue
            rest = behind[c] - weight * pull
            new_behind.append(rest)
            grad = weight * pull - rest * (alpha / (1.0 - alpha))
            ey = ey0 + float(c * rows_chunk)
            gy = grad * ey
            acc[0] = acc[0] + grad
            acc[1] = acc[1] + gy
            acc[2] = acc[2] + gy * ey
            acc[3] = acc[3] + weight * m0
            acc[4] = acc[4] + weight * m1
            acc[5] = acc[5] + weight * m2
        gx = acc[0] * ex
        fields = [acc[0], gx, acc[1], gx * ex, acc[1] * ex, acc[2], acc[3], acc[4], acc[5]]
        packed = zeros
        for j, field in enumerate(fields):
            packed = jnp.where(lane == j, jnp.sum(field, axis=1, keepdims=True), packed)
        sums[spaced, :] = packed
        return new_behind

    lax.fori_loop(0, groups, backward, behinds, unroll=4)

    flat = sums[...].T
    s0, sx, sy, sxx, sxy, syy, d_red, d_green, d_blue = [flat[j : j + 1, :] for j in range(9)]
    d_x = conic_a * sx + conic_b * sy
    d_y = conic_b * sx + conic_c * sy
    d_a, d_b, d_c = -0.5 * sxx, -sxy, -0.5 * syy
    d_xx = -(conic_a * conic_a * d_a + conic_a * conic_b * d_b + conic_b * conic_b * d_c)
    d_yy = -(conic_b * conic_b * d_a + conic_b * conic_c * d_b + conic_c * conic_c * d_c)
    d_xy = -(
        2.0 * conic_a * conic_b * d_a
        + (conic_a * conic_c + conic_b * conic_b) * d_b
        + 2.0 * conic_b * conic_c * d_c
    )
    out = [first[j] * d_x + second[j] * d_y for j in range(3)]
    for j in range(3):
        d_var = first[j] * first[j] * d_xx + first[j] * second[j] * d_xy + second[j] * second[j] * d_yy
        out.append(2.0 * variance[j] * d_var)
    out += [s0 * (1.0 - opacity), d_red, d_green, d_blue]
    out = jnp.concatenate(out, axis=0)
    for j in range(slabs):
        grad_ref[j * 10 : (j + 1) * 10, :] = out[:, j * slab : (j + 1) * slab]

    def grads(step):
        return remote(
            grad_ref, inbox.at[step], grad_send.at[step], grad_recv.at[step], across(step)
        )

    for step in range(tiles - 1, 0, -1):
        grads(step).start()

    def placed(block, slot):
        onehot, mask = entry_names(slot)
        wide = jnp.concatenate([block[j * 10 : (j + 1) * 10, :] for j in range(slabs)], axis=1)
        spots = jnp.concatenate(
            [jnp.where(mask, wide[p : p + 1, :], 0.0) for p in range(10)], axis=0
        )
        high = spots.astype(BF16)
        middle = (spots - high.astype(F32)).astype(BF16)
        dims = (((1,), (1,)), ((), ()))
        return lax.dot_general(
            high, onehot, dims, preferred_element_type=F32
        ) + lax.dot_general(middle, onehot, dims, preferred_element_type=F32)

    partial[...] = placed(grad_ref[...], me_t)

    def add(step):
        grads(step).wait()
        partial[...] += placed(inbox[step], tile_at(step))

    each_tile(add)

    size = lines // 2

    def side(index):
        return pl.ds(pl.multiple_of(index * size, 8), size)

    core = lax.rem(me_d, 2)
    mine, other = side(core), side(1 - core)
    pair = remote(partial.at[other], half_in, pair_send.at[0], pair_recv.at[0], along(1))
    pair.start()
    pair.wait()
    half_sum[...] = partial[mine, :] + half_in[...]
    cuts = [
        remote(half_sum, pieces.at[s], cut_send.at[s], cut_recv.at[s], along(s))
        for s in range(2, depths, 2)
    ]
    for copy in cuts:
        copy.start()
    total = half_sum[...]
    for copy in cuts:
        copy.wait_recv()
    for s in range(2, depths, 2):
        total = total + pieces[s]
    whole_out[mine, :] = total
    share = remote(
        whole_out.at[mine], whole_out.at[mine], pair_send.at[1], pair_recv.at[1], along(1)
    )
    share.start()
    for copy in cuts:
        copy.wait_send()
    for copy in image_copies:
        copy.wait()
    for d in range(depths):
        for k in range(3):
            picture_ref[k, d : d + 1, :] = images_ref[d, k : k + 1, :]
    share.wait()
    for h in range(highs):
        part = slice(h * LANES, (h + 1) * LANES)
        spaced = pl.ds(h, 10, stride=highs)
        new_param_ref[:, part], new_first_ref[:, part], new_second_ref[:, part] = adam_update(
            param_ref[spaced, :], first_ref[:, part], second_ref[:, part], whole_out[spaced, :]
        )


def adam_update(param, first, second, gradient):
    new_first = 0.9 * first + 0.1 * gradient
    new_second = 0.999 * second + 0.001 * gradient * gradient
    corrected = new_first / (1.0 - 0.9**10) / (jnp.sqrt(new_second / (1.0 - 0.999**10)) + 1e-08)
    return (param - 0.05 * corrected, new_first, new_second)


def finish_kernel(*refs):
    count = (len(refs) - 1) // 2
    copies = [
        pltpu.make_async_copy(refs[i], refs[count + i], refs[-1].at[i]) for i in range(count)
    ]
    for copy in copies:
        copy.start()
    for copy in copies:
        copy.wait()


def body(
    positions, log_scales, opacity_logits, colors, first_moment, second_moment,
    cameras, background, target, tile_view, tile_length, list_owner, list_row,
):
    tiles_here, _, pixels = target.shape
    slab = list_row.shape[2]
    depths = lax.axis_size("depth")
    tiles = lax.axis_size("tile")
    entries = slab * depths
    splats = positions.shape[1]
    lines = 10 * splats // LANES
    assert tiles_here == depths and slab == LANES and depths % 2 == 0
    assert tiles & (tiles - 1) == 0 and depths & (depths - 1) == 0
    dma = pltpu.SemaphoreType.DMA
    block = (10 * depths, slab)
    limit = 60 << 20
    args = [
        list_owner.reshape(tiles_here, 1, slab), list_row[0],
        positions, log_scales, opacity_logits, colors, first_moment, second_moment,
        target.transpose(1, 0, 2), tile_view, tile_length, cameras, background,
    ]
    held = [
        (pltpu.VMEM if i < 9 else pltpu.SMEM)(arg.shape, arg.dtype) for i, arg in enumerate(args)
    ]
    results = [(3, tiles_here, pixels)] + [(10, splats)] * 3
    done = pl.pallas_call(
        functools.partial(step_kernel, tiles, depths),
        out_shape=[pltpu.VMEM(shape, F32) for shape in results],
        in_specs=[pl.BlockSpec(memory_space=pl.ANY)] * len(args),
        out_specs=[pl.BlockSpec(memory_space=pltpu.VMEM)] * len(results),
        scratch_shapes=held + [
            dma((len(args),)),
            pltpu.VMEM((depths, 1, slab), jnp.int32),
            pltpu.VMEM((tiles, depths, 1, slab), jnp.int32),
            pltpu.VMEM((lines, LANES), F32),
            pltpu.VMEM((lines, 2 * LANES), BF16),
            pltpu.VMEM((lines, LANES), BF16),
            pltpu.VMEM((tiles,) + block, F32),
            pltpu.VMEM((tiles,) + block, F32),
            dma((tiles, depths)),
            dma((tiles, depths)),
            dma((tiles,)),
            dma((tiles,)),
            pltpu.VMEM((entries, pixels), F32),
            pltpu.VMEM((entries, pixels), F32),
            pltpu.VMEM((3, 8, pixels), F32),
            pltpu.VMEM((8, pixels), F32),
            pltpu.VMEM((entries, LANES), F32),
            pltpu.VMEM((entries, LANES), F32),
            pltpu.VMEM(block, F32),
            pltpu.VMEM((3, pixels), F32),
            pltpu.VMEM((depths, 3, pixels), F32),
            pltpu.VMEM((tiles,) + block, F32),
            pltpu.VMEM((lines, LANES), F32),
            pltpu.VMEM((lines // 2, LANES), F32),
            pltpu.VMEM((lines // 2, LANES), F32),
            pltpu.VMEM((depths, lines // 2, LANES), F32),
            pltpu.VMEM((lines, LANES), F32),
            dma((tiles,)),
            dma((tiles,)),
            dma((depths,)),
            dma((depths,)),
            dma((2,)),
            dma((2,)),
            dma((depths,)),
            dma((depths,)),
            dma((2,)),
            dma((2,)),
        ],
        name="step",
        compiler_params=pltpu.CompilerParams(
            collective_id=1, has_side_effects=True, vmem_limit_bytes=limit
        ),
    )(*args)
    picture, new_params, new_first, new_second = pl.pallas_call(
        finish_kernel,
        out_shape=[jax.ShapeDtypeStruct(shape, F32) for shape in results],
        in_specs=[pl.BlockSpec(memory_space=pltpu.VMEM)] * len(results),
        out_specs=[pl.BlockSpec(memory_space=pl.ANY)] * len(results),
        scratch_shapes=[dma((len(results),))],
        name="finish",
    )(*[pltpu.with_memory_space_constraint(x, pltpu.VMEM) for x in done])
    return (picture.transpose(1, 0, 2), new_params, new_first, new_second)


def solution(mesh):
    placed = (
        P(None, "tile"),
        P(None, "tile"),
        P(None, "tile"),
        P(None, "tile"),
        P(None, "tile"),
        P(None, "tile"),
        P(),
        P(),
        P("tile", None, None),
        P("tile"),
        P("tile"),
        P("depth", "tile", None, None),
        P("depth", "tile", None),
    )
    return jax.shard_map(
        body,
        mesh=mesh,
        in_specs=placed,
        out_specs=(P("tile", None, None), P(None, "tile"), P(None, "tile"), P(None, "tile")),
        check_vma=False,
    )
```

```python
import functools

import jax
import jax.numpy as jnp
from jax import lax
from jax.experimental import pallas as pl
from jax.experimental.pallas import tpu as pltpu
from jax.sharding import PartitionSpec as P

TILE_SIDE = 32
LANES = 128
MESH = pl.DeviceIdType.MESH
F32 = jnp.float32
BF16 = jnp.bfloat16
LOG2E = 1.4426950408889634
PRODUCTS = ((0, 0), (0, 1), (1, 0), (0, 2), (1, 1), (2, 0))
PULL_ROW, PULL_ROWS = 32, 32


def greet(peers):
    barrier = pltpu.get_barrier_semaphore()
    for peer in peers:
        pl.semaphore_signal(barrier, inc=1, device_id=peer, device_id_type=MESH)
    pl.semaphore_wait(barrier, len(peers))


def remote(source, target, send, receive, peer):
    return pltpu.make_async_remote_copy(
        src_ref=source, dst_ref=target, send_sem=send, recv_sem=receive,
        device_id=peer, device_id_type=MESH,
    )


def split3(x):
    high = x.astype(BF16)
    rest = x - high.astype(F32)
    middle = rest.astype(BF16)
    low = (rest - middle.astype(F32)).astype(BF16)
    return high, middle, low


def flip(index, step, size):
    out, bit = 0, 1
    while bit < size:
        mine = lax.rem(lax.div(index, bit), 2)
        if isinstance(step, int):
            out = out + bit * (1 - mine if (step // bit) % 2 else mine)
        else:
            out = out + bit * lax.rem(mine + lax.rem(lax.div(step, bit), 2), 2)
        bit *= 2
    return out


def step_kernel(
    tiles, depths,
    owner_in, row_in, place_in, scale_in, logit_in, color_in, first_in, second_in,
    target_in, view_in, length_in, cam_in, back_in,
    picture_ref, new_param_ref, new_first_ref, new_second_ref,
    owner_ref, row_ref, place_ref, scale_ref, logit_ref, color_ref, first_ref, second_ref,
    target_ref, view_ref, length_ref, cam_ref, back_ref, loads,
    named_ref, lists_ref, param_ref, high_ref, low_ref, answers, got,
    ask_send, ask_recv, send, receive,
    alphas, weights, pulls, misses, carries, columns, ordered, entry_ref, basis_ref, miss_ref,
    sums, grad_ref, image_ref, images_ref,
    inbox, partial, half_in, half_sum, pieces, whole_out,
    grad_send, grad_recv, image_send, image_recv, pair_send, pair_recv, cut_send, cut_recv,
    all_send, all_recv,
):
    lines = param_ref.shape[0]
    highs = lines // 10
    slabs, _, slab = named_ref.shape
    entries = slabs * slab
    pixels = target_ref.shape[2]
    splats = highs * LANES
    me_t, me_d = lax.axis_index("tile"), lax.axis_index("depth")
    small = tiles <= 8
    depth_of = [me_d] + [flip(me_d, b, depths) for b in range(1, depths)]
    tile_of = [me_t] + [flip(me_t, a, tiles) for a in range(1, tiles)] if small else None
    steps = [(a, b) for a in range(tiles - 1, -1, -1) for b in range(depths) if a or b]

    def tile_at(step):
        return tile_of[step] if small else flip(me_t, step, tiles)

    def to(a, b):
        return {"tile": tile_at(a), "depth": depth_of[b]}

    def across(step):
        return {"tile": tile_at(step)}

    def along(step):
        return {"depth": depth_of[step]}

    def each_tile(function):
        if small:
            for step in range(1, tiles):
                function(step)
        else:
            def one(step, carry):
                function(step)
                return carry

            lax.fori_loop(1, tiles, one, 0)

    barrier = pltpu.get_barrier_semaphore()
    for a, b in steps:
        pl.semaphore_signal(barrier, inc=1, device_id=to(a, b), device_id_type=MESH)
    pairs = [
        (owner_in, owner_ref), (row_in, row_ref), (place_in, place_ref), (scale_in, scale_ref),
        (logit_in, logit_ref), (color_in, color_ref), (view_in, view_ref), (length_in, length_ref),
        (cam_in, cam_ref), (back_in, back_ref), (target_in, target_ref),
        (first_in, first_ref), (second_in, second_ref),
    ]
    copies = [
        pltpu.make_async_copy(source, target, loads.at[i])
        for i, (source, target) in enumerate(pairs)
    ]
    for copy in copies:
        copy.start()
    miss_ref[...] = jnp.zeros(miss_ref.shape, BF16)
    spot = lax.broadcasted_iota(jnp.int32, (1, pixels), 1)
    spot_x = (spot & (TILE_SIDE - 1)).astype(F32) + (0.5 - 0.5 * TILE_SIDE)
    spot_y = (spot >> 5).astype(F32) + (0.5 - 0.5 * (pixels // TILE_SIDE))
    parts = [[jnp.ones((1, pixels), F32)], [spot_x], [spot_y]]
    for square in (spot_x * spot_x, spot_x * spot_y, spot_y * spot_y):
        coarse = square.astype(BF16).astype(F32)
        parts.append([coarse, square - coarse])
    rows = [part for piece in parts for _ in range(3) for part in piece]
    rows.append(jnp.zeros((LANES - len(rows), pixels), F32))
    basis_ref[...] = jnp.concatenate(rows, axis=0).astype(BF16)
    for copy in copies[:2]:
        copy.wait()
    for q in range(slabs):
        named_ref[q] = owner_ref[q] * splats + row_ref[q : q + 1, :]
    pl.semaphore_wait(barrier, len(steps))

    def asked(a, b):
        return remote(
            named_ref.at[depth_of[b]], lists_ref.at[me_t, me_d],
            ask_send.at[a, b], ask_recv.at[a, b], to(a, b),
        )

    for a, b in steps:
        asked(a, b).start()
    lists_ref[me_t, me_d] = named_ref[me_d]
    for copy in copies[2:6]:
        copy.wait()
    param = 0
    for ref in (place_ref, scale_ref, logit_ref, color_ref):
        for k in range(ref.shape[0]):
            for h in range(highs):
                line = param * highs + h
                param_ref[line : line + 1, :] = ref[k : k + 1, h * LANES : (h + 1) * LANES]
            param += 1
    high, middle, low = split3(param_ref[...])
    high_ref[...] = jnp.concatenate([high, middle], axis=1)
    low_ref[...] = low
    low_iota = lax.broadcasted_iota(jnp.int32, (LANES, entries), 0)
    high_iota = lax.broadcasted_iota(jnp.int32, (highs, entries), 0) + me_t * highs

    def entry_names(slot):
        names = jnp.concatenate([lists_ref[slot, d] for d in range(slabs)], axis=1)
        onehot = jnp.where(low_iota == (names & (LANES - 1)), 1.0, 0.0).astype(BF16)
        return onehot, high_iota == (names >> 7)

    def answer(slot):
        onehot, mask = entry_names(slot)
        twice = jnp.concatenate([onehot, onehot], axis=0)
        found = jnp.dot(high_ref[...], twice, preferred_element_type=F32) + jnp.dot(
            low_ref[...], onehot, preferred_element_type=F32
        )
        return jnp.concatenate(
            [
                jnp.sum(
                    jnp.where(mask, found[p * highs : (p + 1) * highs], 0.0), axis=0, keepdims=True
                )
                for p in range(10)
            ],
            axis=0,
        )

    def put(ref, step, rows):
        for j in range(slabs):
            ref[step, j * 10 : (j + 1) * 10, :] = rows[:, j * slab : (j + 1) * slab]

    def back(step):
        return remote(
            answers.at[step], got.at[step], send.at[step], receive.at[step], across(step)
        )

    def serve(*group):
        for step in group:
            for b in range(depths):
                asked(step, b).wait_recv()
        for step in group:
            put(answers, step, answer(tile_at(step)))
        for step in group:
            back(step).start()

    for b in range(1, depths):
        asked(0, b).wait_recv()
    put(got, 0, answer(me_t))
    if small:
        for step in range(1, tiles, 2):
            serve(*range(step, min(step + 2, tiles)))
    else:
        each_tile(serve)
    for a, b in steps:
        asked(a, b).wait_send()
    for copy in copies[6:]:
        copy.wait()

    def take(step):
        back(step).wait()
        got[0] += got[step]

    each_tile(take)
    found = got[0]

    chunks = pixels // LANES
    groups = entries // 8
    length = length_ref[me_d]
    view = view_ref[me_d]
    values = [
        jnp.concatenate([found[j * 10 + p : j * 10 + p + 1, :] for j in range(slabs)], axis=1)
        for p in range(10)
    ]

    first = [cam_ref[view, 0, j] for j in range(4)]
    second = [cam_ref[view, 1, j] for j in range(4)]
    variance = [jnp.exp(2.0 * values[3 + j]) for j in range(3)]
    center_x = first[0] * values[0] + first[1] * values[1] + first[2] * values[2] + first[3]
    center_y = second[0] * values[0] + second[1] * values[1] + second[2] * values[2] + second[3]
    cov_xx = sum(first[j] * first[j] * variance[j] for j in range(3)) + 0.3
    cov_xy = sum(first[j] * second[j] * variance[j] for j in range(3))
    cov_yy = sum(second[j] * second[j] * variance[j] for j in range(3)) + 0.3
    determinant = cov_xx * cov_yy - cov_xy * cov_xy
    conic_a = cov_yy / determinant
    conic_b = -cov_xy / determinant
    conic_c = cov_xx / determinant
    fade = 1.0 + jnp.exp(-values[6])
    opacity = 1.0 / fade
    place = lax.broadcasted_iota(jnp.int32, (1, entries), 1)
    slope_x = conic_a * center_x + conic_b * center_y
    slope_y = conic_b * center_x + conic_c * center_y
    level = -0.5 * (slope_x * center_x + slope_y * center_y) - jnp.log(fade)
    terms = [
        jnp.where(place < length, LOG2E * level, -1e30),
        LOG2E * slope_x, LOG2E * slope_y,
        (-0.5 * LOG2E) * conic_a, -LOG2E * conic_b, (-0.5 * LOG2E) * conic_c,
    ]
    rows = []
    for term, copies_of in zip(terms, (1, 1, 1, 2, 2, 2)):
        for piece in split3(term):
            rows += [piece.astype(F32)] * copies_of
    rows += [jnp.zeros((PULL_ROW - len(rows), entries), F32)]
    for k in range(3):
        pieces_of = split3(values[7 + k])
        rows += [pieces_of[i].astype(F32) for i, _ in PRODUCTS]
    rows += values[7:10]
    rows += [jnp.zeros((LANES - PULL_ROW - 3 * len(PRODUCTS) - 3, entries), F32)]
    columns[...] = jnp.concatenate(rows, axis=0).T
    for g in range(groups):
        block = columns[pl.ds(g, 8, stride=groups), :]
        ordered[g * 8 : (g + 1) * 8, :] = block
    entry_ref[...] = ordered[...].astype(BF16)
    width = 2 * LANES
    for n in range(pixels // width):
        part = slice(n * width, (n + 1) * width)
        alphas[:, part] = jnp.exp2(
            jnp.dot(entry_ref[...], basis_ref[:, part], preferred_element_type=F32)
        )

    lane = lax.broadcasted_iota(jnp.int32, (8, LANES), 1)
    sub = lax.broadcasted_iota(jnp.int32, (8, LANES), 0)
    rows_chunk = LANES // TILE_SIDE
    pixel_x = (lane & (TILE_SIDE - 1)).astype(F32) + (0.5 - 0.5 * TILE_SIDE)
    pixel_y = (lane >> 5).astype(F32) - 0.5 * (rows_chunk - 1)
    ones = jnp.ones((8, LANES), F32)
    tint = PULL_ROW + 3 * len(PRODUCTS)

    def spread(cols, j):
        return jnp.broadcast_to(cols[:, j : j + 1], (8, LANES))

    def forward(g, carry):
        trans, color = carry
        at = pl.ds(pl.multiple_of(g * 8, 8), 8)
        cols = ordered[at, :]
        red, green, blue = [spread(cols, tint + j) for j in range(3)]
        new_trans, new_color = [], []
        for c in range(chunks):
            t = trans[c]
            part = slice(c * LANES, (c + 1) * LANES)
            weight = alphas[at, part] * t
            weights[at, part] = weight
            new_trans.append(t - weight)
            new_color.append(color[3 * c] + weight * red)
            new_color.append(color[3 * c + 1] + weight * green)
            new_color.append(color[3 * c + 2] + weight * blue)
        return new_trans, new_color

    zeros = jnp.zeros((8, LANES), F32)
    trans, color = lax.fori_loop(
        0, groups, forward, ([ones] * chunks, [zeros] * (3 * chunks)), unroll=4
    )

    chosen = lax.broadcasted_iota(jnp.int32, (slabs, LANES), 0) == me_d
    behinds = []
    for c in range(chunks):
        part = slice(c * LANES, (c + 1) * LANES)
        run = jnp.where(sub >= 1, pltpu.roll(trans[c], 1, 0), 1.0)
        for s in (1, 2, 4):
            run = run * jnp.where(sub >= s, pltpu.roll(run, s, 0), 1.0)
        carries[:, part] = run
        left = (run * trans[c])[7:8, :]
        pulled = zeros
        last = zeros[0:1]
        for k in range(3):
            shade = jnp.sum(run * color[3 * c + k], axis=0, keepdims=True) + left * back_ref[k]
            image_ref[k : k + 1, part] = shade
            miss = shade - jnp.sum(
                jnp.where(chosen, target_ref[k, :, part], 0.0), axis=0, keepdims=True
            )
            misses[k, :, part] = jnp.broadcast_to(miss, (8, LANES))
            pulled = pulled + miss * color[3 * c + k]
            last = last + miss * back_ref[k]
        kept = trans[c]
        for s in (1, 2, 4):
            inner = sub < 8 - s
            pulled = pulled + kept * jnp.where(inner, pltpu.roll(pulled, 8 - s, 0), 0.0)
            kept = kept * jnp.where(inner, pltpu.roll(kept, 8 - s, 0), 1.0)
        begins = pulled + kept * last
        behinds.append(
            jnp.where(sub < 7, pltpu.roll(begins, 7, 0), jnp.broadcast_to(last, (8, LANES)))
        )
    images_ref[me_d] = image_ref[...]
    image_copies = [
        remote(image_ref, images_ref.at[me_d], image_send.at[s], image_recv.at[s], along(s))
        for s in range(1, depths)
    ]
    for copy in image_copies:
        copy.start()
    rows = []
    for k in range(3):
        pieces_of = split3(misses[k, 0:1, :])
        rows += [pieces_of[j].astype(F32) for _, j in PRODUCTS]
    rows += [jnp.zeros((PULL_ROWS - len(rows), pixels), F32)]
    miss_ref[PULL_ROW : PULL_ROW + PULL_ROWS, :] = jnp.concatenate(rows, axis=0).astype(BF16)
    for n in range(pixels // width):
        part = slice(n * width, (n + 1) * width)
        pulls[:, part] = jnp.dot(entry_ref[...], miss_ref[:, part], preferred_element_type=F32)

    def backward(i, behind):
        g = groups - 1 - i
        at = pl.ds(pl.multiple_of(g * 8, 8), 8)
        new_behind, grad = [], []
        shades = [zeros] * 3
        for c in range(chunks):
            part = slice(c * LANES, (c + 1) * LANES)
            weight = weights[at, part] * carries[:, part]
            gap = pulls[at, part] - behind[c]
            new_behind.append(behind[c] + alphas[at, part] * gap)
            grad.append(weight * gap)
            shades = [shades[k] + weight * misses[k, :, part] for k in range(3)]
        sum_0, sum_1, sum_2 = zeros, zeros, zeros
        for c in range(chunks // 2):
            low, high = grad[c], grad[chunks - 1 - c]
            off = float(rows_chunk) * (0.5 * (chunks - 1) - c)
            even, odd = low + high, high - low
            sum_0 = sum_0 + even
            sum_1 = sum_1 + off * odd
            sum_2 = sum_2 + (off * off) * even
        down = sum_1 + pixel_y * sum_0
        down_2 = sum_2 + pixel_y * (sum_1 + down)
        right = sum_0 * pixel_x
        fields = [sum_0, right, down, right * pixel_x, down * pixel_x, down_2] + shades
        packed = zeros
        for j, field in enumerate(fields):
            packed = jnp.where(lane == j, jnp.sum(field, axis=1, keepdims=True), packed)
        sums[pl.ds(g, 8, stride=groups), :] = packed
        return new_behind

    lax.fori_loop(0, groups, backward, behinds, unroll=4)

    flat = sums[...].T
    s0, sx, sy, sxx, sxy, syy, d_red, d_green, d_blue = [flat[j : j + 1, :] for j in range(9)]
    sxx = sxx - center_x * sx
    sxy = sxy - center_x * sy
    syy = syy - center_y * sy
    sx = sx - center_x * s0
    sy = sy - center_y * s0
    sxx = sxx - center_x * sx
    sxy = sxy - center_y * sx
    syy = syy - center_y * sy
    d_x = conic_a * sx + conic_b * sy
    d_y = conic_b * sx + conic_c * sy
    d_a, d_b, d_c = -0.5 * sxx, -sxy, -0.5 * syy
    d_xx = -(conic_a * conic_a * d_a + conic_a * conic_b * d_b + conic_b * conic_b * d_c)
    d_yy = -(conic_b * conic_b * d_a + conic_b * conic_c * d_b + conic_c * conic_c * d_c)
    d_xy = -(
        2.0 * conic_a * conic_b * d_a
        + (conic_a * conic_c + conic_b * conic_b) * d_b
        + 2.0 * conic_b * conic_c * d_c
    )
    out = [first[j] * d_x + second[j] * d_y for j in range(3)]
    for j in range(3):
        d_var = first[j] * first[j] * d_xx + first[j] * second[j] * d_xy + second[j] * second[j] * d_yy
        out.append(2.0 * variance[j] * d_var)
    out += [s0 * (1.0 - opacity), d_red, d_green, d_blue]
    out = jnp.concatenate(out, axis=0)
    for j in range(slabs):
        grad_ref[j * 10 : (j + 1) * 10, :] = out[:, j * slab : (j + 1) * slab]

    def grads(step):
        return remote(
            grad_ref, inbox.at[step], grad_send.at[step], grad_recv.at[step], across(step)
        )

    for step in range(tiles - 1, 0, -1):
        grads(step).start()

    def placed(block, slot):
        onehot, mask = entry_names(slot)
        wide = jnp.concatenate([block[j * 10 : (j + 1) * 10, :] for j in range(slabs)], axis=1)
        spots = jnp.concatenate(
            [jnp.where(mask, wide[p : p + 1, :], 0.0) for p in range(10)], axis=0
        )
        high = spots.astype(BF16)
        middle = (spots - high.astype(F32)).astype(BF16)
        dims = (((1,), (1,)), ((), ()))
        return lax.dot_general(
            high, onehot, dims, preferred_element_type=F32
        ) + lax.dot_general(middle, onehot, dims, preferred_element_type=F32)

    partial[...] = placed(grad_ref[...], me_t)

    def add(step):
        grads(step).wait()
        partial[...] += placed(inbox[step], tile_at(step))

    each_tile(add)

    size = lines // 2

    def side(index):
        return pl.ds(pl.multiple_of(index * size, 8), size)

    core = lax.rem(me_d, 2)
    mine, other = side(core), side(1 - core)
    pair = remote(partial.at[other], half_in, pair_send.at[0], pair_recv.at[0], along(1))
    pair.start()
    pair.wait()
    half_sum[...] = partial[mine, :] + half_in[...]
    cuts = [
        remote(half_sum, pieces.at[s], cut_send.at[s], cut_recv.at[s], along(s))
        for s in range(2, depths, 2)
    ]
    for copy in cuts:
        copy.start()
    total = half_sum[...]
    for copy in cuts:
        copy.wait_recv()
    for s in range(2, depths, 2):
        total = total + pieces[s]
    whole_out[mine, :] = total
    share = remote(
        whole_out.at[mine], whole_out.at[mine], pair_send.at[1], pair_recv.at[1], along(1)
    )
    share.start()
    for copy in cuts:
        copy.wait_send()
    for copy in image_copies:
        copy.wait()
    for d in range(depths):
        for k in range(3):
            picture_ref[k, d : d + 1, :] = images_ref[d, k : k + 1, :]
    share.wait()
    for h in range(highs):
        part = slice(h * LANES, (h + 1) * LANES)
        spaced = pl.ds(h, 10, stride=highs)
        new_param_ref[:, part], new_first_ref[:, part], new_second_ref[:, part] = adam_update(
            param_ref[spaced, :], first_ref[:, part], second_ref[:, part], whole_out[spaced, :]
        )


def adam_update(param, first, second, gradient):
    new_first = 0.9 * first + 0.1 * gradient
    new_second = 0.999 * second + 0.001 * gradient * gradient
    corrected = new_first / (1.0 - 0.9**10) / (jnp.sqrt(new_second / (1.0 - 0.999**10)) + 1e-08)
    return (param - 0.05 * corrected, new_first, new_second)


def finish_kernel(*refs):
    count = (len(refs) - 1) // 2
    copies = [
        pltpu.make_async_copy(refs[i], refs[count + i], refs[-1].at[i]) for i in range(count)
    ]
    for copy in copies:
        copy.start()
    for copy in copies:
        copy.wait()


def body(
    positions, log_scales, opacity_logits, colors, first_moment, second_moment,
    cameras, background, target, tile_view, tile_length, list_owner, list_row,
):
    tiles_here, _, pixels = target.shape
    slab = list_row.shape[2]
    depths = lax.axis_size("depth")
    tiles = lax.axis_size("tile")
    entries = slab * depths
    splats = positions.shape[1]
    lines = 10 * splats // LANES
    assert tiles_here == depths and slab == LANES and depths % 2 == 0
    assert tiles & (tiles - 1) == 0 and depths & (depths - 1) == 0
    dma = pltpu.SemaphoreType.DMA
    block = (10 * depths, slab)
    limit = 60 << 20
    args = [
        list_owner.reshape(tiles_here, 1, slab), list_row[0],
        positions, log_scales, opacity_logits, colors, first_moment, second_moment,
        target.transpose(1, 0, 2), tile_view, tile_length, cameras, background,
    ]
    held = [
        (pltpu.VMEM if i < 9 else pltpu.SMEM)(arg.shape, arg.dtype) for i, arg in enumerate(args)
    ]
    results = [(3, tiles_here, pixels)] + [(10, splats)] * 3
    done = pl.pallas_call(
        functools.partial(step_kernel, tiles, depths),
        out_shape=[pltpu.VMEM(shape, F32) for shape in results],
        in_specs=[pl.BlockSpec(memory_space=pl.ANY)] * len(args),
        out_specs=[pl.BlockSpec(memory_space=pltpu.VMEM)] * len(results),
        scratch_shapes=held + [
            dma((len(args),)),
            pltpu.VMEM((depths, 1, slab), jnp.int32),
            pltpu.VMEM((tiles, depths, 1, slab), jnp.int32),
            pltpu.VMEM((lines, LANES), F32),
            pltpu.VMEM((lines, 2 * LANES), BF16),
            pltpu.VMEM((lines, LANES), BF16),
            pltpu.VMEM((tiles,) + block, F32),
            pltpu.VMEM((tiles,) + block, F32),
            dma((tiles, depths)),
            dma((tiles, depths)),
            dma((tiles,)),
            dma((tiles,)),
            pltpu.VMEM((entries, pixels), F32),
            pltpu.VMEM((entries, pixels), F32),
            pltpu.VMEM((entries, pixels), F32),
            pltpu.VMEM((3, 8, pixels), F32),
            pltpu.VMEM((8, pixels), F32),
            pltpu.VMEM((entries, LANES), F32),
            pltpu.VMEM((entries, LANES), F32),
            pltpu.VMEM((entries, LANES), BF16),
            pltpu.VMEM((LANES, pixels), BF16),
            pltpu.VMEM((LANES, pixels), BF16),
            pltpu.VMEM((entries, LANES), F32),
            pltpu.VMEM(block, F32),
            pltpu.VMEM((3, pixels), F32),
            pltpu.VMEM((depths, 3, pixels), F32),
            pltpu.VMEM((tiles,) + block, F32),
            pltpu.VMEM((lines, LANES), F32),
            pltpu.VMEM((lines // 2, LANES), F32),
            pltpu.VMEM((lines // 2, LANES), F32),
            pltpu.VMEM((depths, lines // 2, LANES), F32),
            pltpu.VMEM((lines, LANES), F32),
            dma((tiles,)),
            dma((tiles,)),
            dma((depths,)),
            dma((depths,)),
            dma((2,)),
            dma((2,)),
            dma((depths,)),
            dma((depths,)),
            dma((2,)),
            dma((2,)),
        ],
        name="step",
        compiler_params=pltpu.CompilerParams(
            collective_id=1, has_side_effects=True, vmem_limit_bytes=limit
        ),
    )(*args)
    picture, new_params, new_first, new_second = pl.pallas_call(
        finish_kernel,
        out_shape=[jax.ShapeDtypeStruct(shape, F32) for shape in results],
        in_specs=[pl.BlockSpec(memory_space=pltpu.VMEM)] * len(results),
        out_specs=[pl.BlockSpec(memory_space=pl.ANY)] * len(results),
        scratch_shapes=[dma((len(results),))],
        name="finish",
    )(*[pltpu.with_memory_space_constraint(x, pltpu.VMEM) for x in done])
    return (picture.transpose(1, 0, 2), new_params, new_first, new_second)


def solution(mesh):
    placed = (
        P(None, "tile"),
        P(None, "tile"),
        P(None, "tile"),
        P(None, "tile"),
        P(None, "tile"),
        P(None, "tile"),
        P(),
        P(),
        P("tile", None, None),
        P("tile"),
        P("tile"),
        P("depth", "tile", None, None),
        P("depth", "tile", None),
    )
    return jax.shard_map(
        body,
        mesh=mesh,
        in_specs=placed,
        out_specs=(P("tile", None, None), P(None, "tile"), P(None, "tile"), P(None, "tile")),
        check_vma=False,
    )
```

```python
import functools

import jax
import jax.numpy as jnp
from jax import lax
from jax.experimental import pallas as pl
from jax.experimental.pallas import tpu as pltpu
from jax.sharding import PartitionSpec as P

TILE_SIDE = 32
LANES = 128
MESH = pl.DeviceIdType.MESH
F32 = jnp.float32
BF16 = jnp.bfloat16
LOG2E = 1.4426950408889634
PRODUCTS = ((0, 0), (0, 1), (1, 0), (0, 2), (1, 1), (2, 0))
PULL_ROW, PULL_ROWS = 32, 32
UNROLL = 16


def greet(peers):
    barrier = pltpu.get_barrier_semaphore()
    for peer in peers:
        pl.semaphore_signal(barrier, inc=1, device_id=peer, device_id_type=MESH)
    pl.semaphore_wait(barrier, len(peers))


def remote(source, target, send, receive, peer):
    return pltpu.make_async_remote_copy(
        src_ref=source, dst_ref=target, send_sem=send, recv_sem=receive,
        device_id=peer, device_id_type=MESH,
    )


def split3(x):
    high = x.astype(BF16)
    rest = x - high.astype(F32)
    middle = rest.astype(BF16)
    low = (rest - middle.astype(F32)).astype(BF16)
    return high, middle, low


def flip(index, step, size):
    out, bit = 0, 1
    while bit < size:
        mine = lax.rem(lax.div(index, bit), 2)
        if isinstance(step, int):
            out = out + bit * (1 - mine if (step // bit) % 2 else mine)
        else:
            out = out + bit * lax.rem(mine + lax.rem(lax.div(step, bit), 2), 2)
        bit *= 2
    return out


def step_kernel(
    tiles, depths,
    owner_in, row_in, place_in, scale_in, logit_in, color_in, first_in, second_in,
    target_in, view_in, length_in, cam_in, back_in,
    picture_ref, new_param_ref, new_first_ref, new_second_ref,
    owner_ref, row_ref, place_ref, scale_ref, logit_ref, color_ref, first_ref, second_ref,
    target_ref, view_ref, length_ref, cam_ref, back_ref, loads,
    named_ref, lists_ref, twin_ref, hot_ref, high_names, first_lines, second_lines, twin_sem,
    param_ref, high_ref, low_ref, answers, got,
    ask_send, ask_recv, send, receive,
    alphas, weights, pulls, misses, carries, columns, ordered, entry_ref, basis_ref, miss_ref,
    sums, grad_ref, image_ref, images_ref,
    inbox, partial, pieces, whole_out,
    grad_send, grad_recv, image_send, image_recv, cut_send, cut_recv, pair_sem,
):
    lines = param_ref.shape[0]
    highs = lines // 10
    slabs, _, slab = named_ref.shape
    entries = slabs * slab
    pixels = target_ref.shape[2]
    splats = highs * LANES
    me_t, me_d = lax.axis_index("tile"), lax.axis_index("depth")
    small = tiles <= 8
    depth_of = [me_d] + [flip(me_d, b, depths) for b in range(1, depths)]
    tile_of = [me_t] + [flip(me_t, a, tiles) for a in range(1, tiles)] if small else None
    steps = [(a, b) for a in range(tiles - 1, -1, -1) for b in range(depths) if a or b]

    def tile_at(step):
        return tile_of[step] if small else flip(me_t, step, tiles)

    def to(a, b):
        return {"tile": tile_at(a), "depth": depth_of[b]}

    def across(step):
        return {"tile": tile_at(step)}

    def along(step):
        return {"depth": depth_of[step]}

    def each_tile(function):
        if small:
            for step in range(1, tiles):
                function(step)
        else:
            def one(step, carry):
                function(step)
                return carry

            lax.fori_loop(1, tiles, one, 0)

    barrier = pltpu.get_barrier_semaphore()
    for a, b in steps:
        pl.semaphore_signal(barrier, inc=1, device_id=to(a, b), device_id_type=MESH)
    pairs = [
        (owner_in, owner_ref), (row_in, row_ref), (place_in, place_ref), (scale_in, scale_ref),
        (logit_in, logit_ref), (color_in, color_ref), (view_in, view_ref), (length_in, length_ref),
        (cam_in, cam_ref), (back_in, back_ref), (target_in, target_ref),
        (first_in, first_ref), (second_in, second_ref),
    ]
    copies = [
        pltpu.make_async_copy(source, target, loads.at[i])
        for i, (source, target) in enumerate(pairs)
    ]
    for copy in copies:
        copy.start()
    miss_ref[...] = jnp.zeros(miss_ref.shape, BF16)
    spot = lax.broadcasted_iota(jnp.int32, (1, pixels), 1)
    spot_x = (spot & (TILE_SIDE - 1)).astype(F32) + (0.5 - 0.5 * TILE_SIDE)
    spot_y = (spot >> 5).astype(F32) + (0.5 - 0.5 * (pixels // TILE_SIDE))
    parts = [[jnp.ones((1, pixels), F32)], [spot_x], [spot_y]]
    for square in (spot_x * spot_x, spot_x * spot_y, spot_y * spot_y):
        coarse = square.astype(BF16).astype(F32)
        parts.append([coarse, square - coarse])
    rows = [part for piece in parts for _ in range(3) for part in piece]
    rows.append(jnp.zeros((LANES - len(rows), pixels), F32))
    basis_ref[...] = jnp.concatenate(rows, axis=0).astype(BF16)
    for copy in copies[:2]:
        copy.wait()
    names = jnp.concatenate([owner_ref[q] for q in range(slabs)], axis=0) * splats + row_ref[...]
    quad = lax.broadcasted_iota(jnp.int32, names.shape, 1) >> ((slab // 4).bit_length() - 1)
    names = jnp.where(
        quad == 1, pltpu.roll(names, 3 * slab // 4, 1),
        jnp.where(quad == 2, pltpu.roll(names, slab // 4, 1), names),
    )
    for q in range(slabs):
        named_ref[q] = names[q : q + 1, :]
    pl.semaphore_wait(barrier, len(steps))

    def asked(a, b):
        return remote(
            named_ref.at[depth_of[b]], lists_ref.at[me_t, me_d],
            ask_send.at[a, b], ask_recv.at[a, b], to(a, b),
        )

    for a, b in steps:
        asked(a, b).start()
    lists_ref[me_t, me_d] = named_ref[me_d]
    for copy in copies[2:6]:
        copy.wait()
    param = 0
    for ref in (place_ref, scale_ref, logit_ref, color_ref):
        for k in range(ref.shape[0]):
            for h in range(highs):
                line = param * highs + h
                param_ref[line : line + 1, :] = ref[k : k + 1, h * LANES : (h + 1) * LANES]
            param += 1
    high, middle, low = split3(param_ref[...])
    high_ref[...] = jnp.concatenate([high, middle], axis=1)
    low_ref[...] = low
    low_iota = lax.broadcasted_iota(jnp.int32, (LANES, entries), 0)
    high_iota = lax.broadcasted_iota(jnp.int32, (highs, entries), 0) + me_t * highs
    span = entries // 2
    early = lax.broadcasted_iota(jnp.int32, (1, slab), 1) < slab // 2

    def widen(ref, slot):
        slab_names = [ref[slot, d] for d in range(slabs)]
        turned = [pltpu.roll(x, slab // 2, 1) for x in slab_names]
        return [
            jnp.where(early, slab_names[d], turned[d + 1]) for d in range(0, slabs, 2)
        ] + [
            jnp.where(early, turned[d], slab_names[d + 1]) for d in range(0, slabs, 2)
        ]

    def marks(names):
        onehot = jnp.where(low_iota == (names & (LANES - 1)), 1.0, 0.0).astype(BF16)
        return onehot, high_iota == (names >> 7)

    def note(source, step, names):
        onehot, mask = marks(names)
        for part in range(2):
            cut = slice(part * span, (part + 1) * span)
            hot_ref[source, step, part] = onehot[:, cut]
            high_names[source, step, part] = names[:, cut] >> 7
        return onehot, mask

    def answer(step):
        onehot, mask = note(0, step, jnp.concatenate(widen(lists_ref, tile_at(step)), axis=1))
        twice = jnp.concatenate([onehot, onehot], axis=0)
        found = jnp.dot(high_ref[...], twice, preferred_element_type=F32) + jnp.dot(
            low_ref[...], onehot, preferred_element_type=F32
        )
        return jnp.concatenate(
            [
                jnp.sum(
                    jnp.where(mask, found[p * highs : (p + 1) * highs], 0.0), axis=0, keepdims=True
                )
                for p in range(10)
            ],
            axis=0,
        )

    def put(ref, step, rows):
        for j in range(slabs):
            k = j % (slabs // 2)
            ref[step, j // (slabs // 2), k * 10 : (k + 1) * 10, :] = rows[
                :, j * slab : (j + 1) * slab
            ]

    def back(step, part):
        return remote(
            answers.at[step, part], got.at[step, part], send.at[step, part],
            receive.at[step, part], across(step),
        )

    def serve(*group):
        for step in group:
            for b in range(depths):
                asked(step, b).wait_recv()
        for step in group:
            put(answers, step, answer(step))
        for step in group:
            back(step, 0).start()

    for b in range(1, depths):
        asked(0, b).wait_recv()
    put(got, 0, answer(0))
    if small:
        for step in range(1, tiles, 2):
            serve(*range(step, min(step + 2, tiles)))
    else:
        each_tile(serve)
    each_tile(lambda step: back(step, 1).start())
    twin = remote(lists_ref, twin_ref, twin_sem.at[0], twin_sem.at[1], along(1))
    twin.start()
    for a, b in steps:
        asked(a, b).wait_send()
    for copy in copies[6:]:
        copy.wait()
    for h in range(highs):
        spaced = pl.ds(h, 10, stride=highs)
        first_lines[spaced, :] = first_ref[:, h * LANES : (h + 1) * LANES]
        second_lines[spaced, :] = second_ref[:, h * LANES : (h + 1) * LANES]
    twin.wait()

    def note_twin(step):
        note(1, step, jnp.concatenate(widen(twin_ref, tile_at(step)), axis=1))

    note_twin(0)
    each_tile(note_twin)

    chunks = pixels // LANES
    groups = entries // 8
    length = length_ref[me_d]
    view = view_ref[me_d]

    first = [cam_ref[view, 0, j] for j in range(4)]
    second = [cam_ref[view, 1, j] for j in range(4)]
    width = 2 * LANES

    def project(part):
        def take(step):
            back(step, part).wait()
            got[0, part] += got[step, part]

        each_tile(take)
        found = got[0, part]
        values = [
            jnp.concatenate(
                [found[j * 10 + p : j * 10 + p + 1, :] for j in range(slabs // 2)], axis=1
            )
            for p in range(10)
        ]
        variance = [jnp.exp(2.0 * values[3 + j]) for j in range(3)]
        center_x = first[0] * values[0] + first[1] * values[1] + first[2] * values[2] + first[3]
        center_y = second[0] * values[0] + second[1] * values[1] + second[2] * values[2] + second[3]
        cov_xx = sum(first[j] * first[j] * variance[j] for j in range(3)) + 0.3
        cov_xy = sum(first[j] * second[j] * variance[j] for j in range(3))
        cov_yy = sum(second[j] * second[j] * variance[j] for j in range(3)) + 0.3
        determinant = cov_xx * cov_yy - cov_xy * cov_xy
        conic_a = cov_yy / determinant
        conic_b = -cov_xy / determinant
        conic_c = cov_xx / determinant
        fade = 1.0 + jnp.exp(-values[6])
        opacity = 1.0 / fade
        spot = lax.broadcasted_iota(jnp.int32, (1, span), 1)
        stretch = groups // 2
        place = (
            (spot >> (stretch.bit_length() - 1)) * groups + part * stretch + (spot & (stretch - 1))
        )
        slope_x = conic_a * center_x + conic_b * center_y
        slope_y = conic_b * center_x + conic_c * center_y
        level = -0.5 * (slope_x * center_x + slope_y * center_y) - jnp.log(fade)
        terms = [
            jnp.where(place < length, LOG2E * level, -1e30),
            LOG2E * slope_x, LOG2E * slope_y,
            (-0.5 * LOG2E) * conic_a, -LOG2E * conic_b, (-0.5 * LOG2E) * conic_c,
        ]
        rows = []
        for term, copies_of in zip(terms, (1, 1, 1, 2, 2, 2)):
            for piece in split3(term):
                rows += [piece.astype(F32)] * copies_of
        rows += [jnp.zeros((PULL_ROW - len(rows), span), F32)]
        for k in range(3):
            pieces_of = split3(values[7 + k])
            rows += [pieces_of[i].astype(F32) for i, _ in PRODUCTS]
        rows += values[7:10]
        rows += [jnp.zeros((LANES - PULL_ROW - 3 * len(PRODUCTS) - 3, span), F32)]
        base = part * span
        columns[base : base + span, :] = jnp.concatenate(rows, axis=0).T
        for g in range(stretch):
            ordered[base + g * 8 : base + (g + 1) * 8, :] = columns[
                pl.ds(base + g, 8, stride=stretch), :
            ]
        entry_ref[base : base + span, :] = ordered[base : base + span, :].astype(BF16)
        for n in range(pixels // width):
            cut = slice(n * width, (n + 1) * width)
            alphas[base : base + span, cut] = jnp.exp2(
                jnp.dot(
                    entry_ref[base : base + span, :], basis_ref[:, cut], preferred_element_type=F32
                )
            )
        return variance, center_x, center_y, conic_a, conic_b, conic_c, opacity

    lane = lax.broadcasted_iota(jnp.int32, (8, LANES), 1)
    sub = lax.broadcasted_iota(jnp.int32, (8, LANES), 0)
    rows_chunk = LANES // TILE_SIDE
    pixel_x = (lane & (TILE_SIDE - 1)).astype(F32) + (0.5 - 0.5 * TILE_SIDE)
    pixel_y = (lane >> 5).astype(F32) - 0.5 * (rows_chunk - 1)
    ones = jnp.ones((8, LANES), F32)
    tint = PULL_ROW + 3 * len(PRODUCTS)

    def spread(cols, j):
        return jnp.broadcast_to(cols[:, j : j + 1], (8, LANES))

    def forward(g, carry):
        trans, color = carry
        at = pl.ds(pl.multiple_of(g * 8, 8), 8)
        cols = ordered[at, :]
        red, green, blue = [spread(cols, tint + j) for j in range(3)]
        new_trans, new_color = [], []
        for c in range(chunks):
            t = trans[c]
            part = slice(c * LANES, (c + 1) * LANES)
            weight = alphas[at, part] * t
            weights[at, part] = weight
            new_trans.append(t - weight)
            new_color.append(color[3 * c] + weight * red)
            new_color.append(color[3 * c + 1] + weight * green)
            new_color.append(color[3 * c + 2] + weight * blue)
        return new_trans, new_color

    zeros = jnp.zeros((8, LANES), F32)
    carried = ([ones] * chunks, [zeros] * (3 * chunks))
    screens = []
    for part in range(2):
        screens.append(project(part))
        carried = lax.fori_loop(
            part * (groups // 2), (part + 1) * (groups // 2), forward, carried, unroll=UNROLL
        )
    trans, color = carried

    chosen = lax.broadcasted_iota(jnp.int32, (slabs, LANES), 0) == me_d
    behinds = []
    for c in range(chunks):
        part = slice(c * LANES, (c + 1) * LANES)
        run = jnp.where(sub >= 1, pltpu.roll(trans[c], 1, 0), 1.0)
        for s in (1, 2, 4):
            run = run * jnp.where(sub >= s, pltpu.roll(run, s, 0), 1.0)
        carries[:, part] = run
        left = (run * trans[c])[7:8, :]
        pulled = zeros
        last = zeros[0:1]
        for k in range(3):
            shade = jnp.sum(run * color[3 * c + k], axis=0, keepdims=True) + left * back_ref[k]
            image_ref[k : k + 1, part] = shade
            miss = shade - jnp.sum(
                jnp.where(chosen, target_ref[k, :, part], 0.0), axis=0, keepdims=True
            )
            misses[k, :, part] = jnp.broadcast_to(miss, (8, LANES))
            pulled = pulled + miss * color[3 * c + k]
            last = last + miss * back_ref[k]
        kept = trans[c]
        for s in (1, 2, 4):
            inner = sub < 8 - s
            pulled = pulled + kept * jnp.where(inner, pltpu.roll(pulled, 8 - s, 0), 0.0)
            kept = kept * jnp.where(inner, pltpu.roll(kept, 8 - s, 0), 1.0)
        begins = pulled + kept * last
        behinds.append(
            jnp.where(sub < 7, pltpu.roll(begins, 7, 0), jnp.broadcast_to(last, (8, LANES)))
        )
    images_ref[me_d] = image_ref[...]
    image_copies = [
        remote(image_ref, images_ref.at[me_d], image_send.at[s], image_recv.at[s], along(s))
        for s in range(1, depths)
    ]
    for copy in image_copies:
        copy.start()
    rows = []
    for k in range(3):
        pieces_of = split3(misses[k, 0:1, :])
        rows += [pieces_of[j].astype(F32) for _, j in PRODUCTS]
    rows += [jnp.zeros((PULL_ROWS - len(rows), pixels), F32)]
    miss_ref[PULL_ROW : PULL_ROW + PULL_ROWS, :] = jnp.concatenate(rows, axis=0).astype(BF16)
    for n in range(pixels // width):
        part = slice(n * width, (n + 1) * width)
        pulls[:, part] = jnp.dot(entry_ref[...], miss_ref[:, part], preferred_element_type=F32)

    def backward(g, behind, piece):
        at = pl.ds(pl.multiple_of(g * 8, 8), 8)
        new_behind, grad = [], []
        shades = [zeros] * 3
        for c in range(chunks):
            part = slice(c * LANES, (c + 1) * LANES)
            weight = weights[at, part] * carries[:, part]
            gap = pulls[at, part] - behind[c]
            new_behind.append(behind[c] + alphas[at, part] * gap)
            grad.append(weight * gap)
            shades = [shades[k] + weight * misses[k, :, part] for k in range(3)]
        sum_0, sum_1, sum_2 = zeros, zeros, zeros
        for c in range(chunks // 2):
            low, high = grad[c], grad[chunks - 1 - c]
            off = float(rows_chunk) * (0.5 * (chunks - 1) - c)
            even, odd = low + high, high - low
            sum_0 = sum_0 + even
            sum_1 = sum_1 + off * odd
            sum_2 = sum_2 + (off * off) * even
        down = sum_1 + pixel_y * sum_0
        down_2 = sum_2 + pixel_y * (sum_1 + down)
        right = sum_0 * pixel_x
        fields = [sum_0, right, down, right * pixel_x, down * pixel_x, down_2] + shades
        packed = zeros
        for j, field in enumerate(fields):
            packed = jnp.where(lane == j, jnp.sum(field, axis=1, keepdims=True), packed)
        stretch = groups // 2
        sums[pl.ds(piece * (span - stretch) + g, 8, stride=stretch), :] = packed
        return new_behind

    core = lax.rem(me_d, 2)

    def grads(step, other, part):
        return remote(
            grad_ref.at[part, core if not other else 1 - core], inbox.at[step, other, part],
            grad_send.at[step, other, part], grad_recv.at[step, other, part],
            to(step, other),
        )

    ways = [(step, other) for step in range(tiles - 1, -1, -1) for other in (0, 1) if step or other]
    for part in (1, 0):
        top = (part + 1) * (groups // 2)
        behinds = lax.fori_loop(
            0, groups // 2, lambda i, behind: backward(top - 1 - i, behind, part), behinds,
            unroll=UNROLL,
        )
        variance, center_x, center_y, conic_a, conic_b, conic_c, opacity = screens[part]
        flat = sums[part * span : (part + 1) * span, :].T
        s0, sx, sy, sxx, sxy, syy, d_red, d_green, d_blue = [flat[j : j + 1, :] for j in range(9)]
        sxx = sxx - center_x * sx
        sxy = sxy - center_x * sy
        syy = syy - center_y * sy
        sx = sx - center_x * s0
        sy = sy - center_y * s0
        sxx = sxx - center_x * sx
        sxy = sxy - center_y * sx
        syy = syy - center_y * sy
        d_x = conic_a * sx + conic_b * sy
        d_y = conic_b * sx + conic_c * sy
        d_a, d_b, d_c = -0.5 * sxx, -sxy, -0.5 * syy
        d_xx = -(conic_a * conic_a * d_a + conic_a * conic_b * d_b + conic_b * conic_b * d_c)
        d_yy = -(conic_b * conic_b * d_a + conic_b * conic_c * d_b + conic_c * conic_c * d_c)
        d_xy = -(
            2.0 * conic_a * conic_b * d_a
            + (conic_a * conic_c + conic_b * conic_b) * d_b
            + 2.0 * conic_b * conic_c * d_c
        )
        out = [first[j] * d_x + second[j] * d_y for j in range(3)]
        for j in range(3):
            d_var = first[j] * first[j] * d_xx + first[j] * second[j] * d_xy + second[j] * second[j] * d_yy
            out.append(2.0 * variance[j] * d_var)
        out += [s0 * (1.0 - opacity), d_red, d_green, d_blue]
        out = jnp.concatenate(out, axis=0)
        for u in range(2):
            for j in range(slabs // 2):
                grad_ref[part, u, j * 5 : (j + 1) * 5, :] = out[
                    u * 5 : (u + 1) * 5, j * slab : (j + 1) * slab
                ]
        for step, other in ways:
            grads(step, other, part).start()

    size = lines // 2

    def placed(blocks, step, part):
        dims = (((1,), (1,)), ((), ()))
        total = 0.0
        for source, block in enumerate(blocks):
            wide = jnp.concatenate(
                [block[j * 5 : (j + 1) * 5, :] for j in range(slabs // 2)], axis=1
            )
            mask = high_iota[:, :span] == high_names[source, step, part]
            high = wide.astype(BF16).astype(F32)
            for rows in (high, wide - high):
                spots = jnp.concatenate(
                    [jnp.where(mask, rows[p : p + 1, :], 0.0) for p in range(5)], axis=0
                )
                total = total + lax.dot_general(
                    spots.astype(BF16), hot_ref[source, step, part], dims,
                    preferred_element_type=F32,
                )
        return total

    partial[...] = jnp.zeros(partial.shape, F32)
    for part in (1, 0):
        grads(0, 1, part).wait()
        partial[...] += placed([grad_ref[part, core], inbox[0, 1, part]], 0, part)

        def add(step):
            for other in (0, 1):
                grads(step, other, part).wait()
            partial[...] += placed([inbox[step, 0, part], inbox[step, 1, part]], step, part)

        each_tile(add)

    def side(index):
        return pl.ds(pl.multiple_of(index * size, 8), size)

    mine = side(core)
    cuts = [
        remote(partial, pieces.at[s], cut_send.at[s], cut_recv.at[s], along(s))
        for s in range(2, depths, 2)
    ]
    for copy in cuts:
        copy.start()
    total = partial[...]
    for copy in cuts:
        copy.wait_recv()
    for s in range(2, depths, 2):
        total = total + pieces[s]
    whole_out[mine, :] = total
    share = remote(
        whole_out.at[mine], whole_out.at[mine], pair_sem.at[0], pair_sem.at[1], along(1)
    )
    share.start()

    def finish(rows):
        param_ref[rows, :], first_lines[rows, :], second_lines[rows, :] = adam_update(
            param_ref[rows, :], first_lines[rows, :], second_lines[rows, :], whole_out[rows, :]
        )

    finish(mine)
    for copy in cuts:
        copy.wait_send()
    for copy in image_copies:
        copy.wait()
    for d in range(depths):
        for k in range(3):
            picture_ref[k, d : d + 1, :] = images_ref[d, k : k + 1, :]
    share.wait()
    finish(side(1 - core))
    for h in range(highs):
        part = slice(h * LANES, (h + 1) * LANES)
        spaced = pl.ds(h, 10, stride=highs)
        new_param_ref[:, part] = param_ref[spaced, :]
        new_first_ref[:, part] = first_lines[spaced, :]
        new_second_ref[:, part] = second_lines[spaced, :]


def adam_update(param, first, second, gradient):
    new_first = 0.9 * first + 0.1 * gradient
    new_second = 0.999 * second + 0.001 * gradient * gradient
    corrected = new_first / (1.0 - 0.9**10) / (jnp.sqrt(new_second / (1.0 - 0.999**10)) + 1e-08)
    return (param - 0.05 * corrected, new_first, new_second)


def finish_kernel(*refs):
    count = (len(refs) - 1) // 2
    copies = [
        pltpu.make_async_copy(refs[i], refs[count + i], refs[-1].at[i]) for i in range(count)
    ]
    for copy in copies:
        copy.start()
    for copy in copies:
        copy.wait()


def body(
    positions, log_scales, opacity_logits, colors, first_moment, second_moment,
    cameras, background, target, tile_view, tile_length, list_owner, list_row,
):
    tiles_here, _, pixels = target.shape
    slab = list_row.shape[2]
    depths = lax.axis_size("depth")
    tiles = lax.axis_size("tile")
    entries = slab * depths
    splats = positions.shape[1]
    lines = 10 * splats // LANES
    assert tiles_here == depths == 4 and slab == LANES
    assert tiles & (tiles - 1) == 0 and depths & (depths - 1) == 0
    dma = pltpu.SemaphoreType.DMA
    block = (5 * depths, slab)
    slip = (5 * depths // 2, slab)
    limit = 60 << 20
    args = [
        list_owner.reshape(tiles_here, 1, slab), list_row[0],
        positions, log_scales, opacity_logits, colors, first_moment, second_moment,
        target.transpose(1, 0, 2), tile_view, tile_length, cameras, background,
    ]
    held = [
        (pltpu.VMEM if i < 9 else pltpu.SMEM)(arg.shape, arg.dtype) for i, arg in enumerate(args)
    ]
    results = [(3, tiles_here, pixels)] + [(10, splats)] * 3
    done = pl.pallas_call(
        functools.partial(step_kernel, tiles, depths),
        out_shape=[pltpu.VMEM(shape, F32) for shape in results],
        in_specs=[pl.BlockSpec(memory_space=pl.ANY)] * len(args),
        out_specs=[pl.BlockSpec(memory_space=pltpu.VMEM)] * len(results),
        scratch_shapes=held + [
            dma((len(args),)),
            pltpu.VMEM((depths, 1, slab), jnp.int32),
            pltpu.VMEM((tiles, depths, 1, slab), jnp.int32),
            pltpu.VMEM((tiles, depths, 1, slab), jnp.int32),
            pltpu.VMEM((2, tiles, 2, LANES, entries // 2), BF16),
            pltpu.VMEM((2, tiles, 2, 1, entries // 2), jnp.int32),
            pltpu.VMEM((lines, LANES), F32),
            pltpu.VMEM((lines, LANES), F32),
            dma((2,)),
            pltpu.VMEM((lines, LANES), F32),
            pltpu.VMEM((lines, 2 * LANES), BF16),
            pltpu.VMEM((lines, LANES), BF16),
            pltpu.VMEM((tiles, 2) + block, F32),
            pltpu.VMEM((tiles, 2) + block, F32),
            dma((tiles, depths)),
            dma((tiles, depths)),
            dma((tiles, 2)),
            dma((tiles, 2)),
            pltpu.VMEM((entries, pixels), F32),
            pltpu.VMEM((entries, pixels), F32),
            pltpu.VMEM((entries, pixels), F32),
            pltpu.VMEM((3, 8, pixels), F32),
            pltpu.VMEM((8, pixels), F32),
            pltpu.VMEM((entries, LANES), F32),
            pltpu.VMEM((entries, LANES), F32),
            pltpu.VMEM((entries, LANES), BF16),
            pltpu.VMEM((LANES, pixels), BF16),
            pltpu.VMEM((LANES, pixels), BF16),
            pltpu.VMEM((entries, LANES), F32),
            pltpu.VMEM((2, 2) + slip, F32),
            pltpu.VMEM((3, pixels), F32),
            pltpu.VMEM((depths, 3, pixels), F32),
            pltpu.VMEM((tiles, 2, 2) + slip, F32),
            pltpu.VMEM((lines // 2, LANES), F32),
            pltpu.VMEM((depths, lines // 2, LANES), F32),
            pltpu.VMEM((lines, LANES), F32),
            dma((tiles, 2, 2)),
            dma((tiles, 2, 2)),
            dma((depths,)),
            dma((depths,)),
            dma((depths,)),
            dma((depths,)),
            dma((2,)),
        ],
        name="step",
        compiler_params=pltpu.CompilerParams(
            collective_id=1, has_side_effects=True, vmem_limit_bytes=limit
        ),
    )(*args)
    picture, new_params, new_first, new_second = pl.pallas_call(
        finish_kernel,
        out_shape=[jax.ShapeDtypeStruct(shape, F32) for shape in results],
        in_specs=[pl.BlockSpec(memory_space=pltpu.VMEM)] * len(results),
        out_specs=[pl.BlockSpec(memory_space=pl.ANY)] * len(results),
        scratch_shapes=[dma((len(results),))],
        name="finish",
    )(*[pltpu.with_memory_space_constraint(x, pltpu.VMEM) for x in done])
    return (picture.transpose(1, 0, 2), new_params, new_first, new_second)


def solution(mesh):
    placed = (
        P(None, "tile"),
        P(None, "tile"),
        P(None, "tile"),
        P(None, "tile"),
        P(None, "tile"),
        P(None, "tile"),
        P(),
        P(),
        P("tile", None, None),
        P("tile"),
        P("tile"),
        P("depth", "tile", None, None),
        P("depth", "tile", None),
    )
    return jax.shard_map(
        body,
        mesh=mesh,
        in_specs=placed,
        out_specs=(P("tile", None, None), P(None, "tile"), P(None, "tile"), P(None, "tile")),
        check_vma=False,
    )
```

```python
import functools

import jax
import jax.numpy as jnp
from jax import lax
from jax.experimental import pallas as pl
from jax.experimental.pallas import tpu as pltpu
from jax.sharding import PartitionSpec as P

TILE_SIDE = 32
LANES = 128
MESH = pl.DeviceIdType.MESH
F32 = jnp.float32
BF16 = jnp.bfloat16
LOG2E = 1.4426950408889634
PRODUCTS = ((0, 0), (0, 1), (1, 0), (0, 2), (1, 1), (2, 0))
PULL_ROW, PULL_ROWS = 32, 32
AHEAD, BACK = 8, 32


def greet(peers):
    barrier = pltpu.get_barrier_semaphore()
    for peer in peers:
        pl.semaphore_signal(barrier, inc=1, device_id=peer, device_id_type=MESH)
    pl.semaphore_wait(barrier, len(peers))


def remote(source, target, send, receive, peer):
    return pltpu.make_async_remote_copy(
        src_ref=source, dst_ref=target, send_sem=send, recv_sem=receive,
        device_id=peer, device_id_type=MESH,
    )


def split3(x):
    high = x.astype(BF16)
    rest = x - high.astype(F32)
    middle = rest.astype(BF16)
    low = (rest - middle.astype(F32)).astype(BF16)
    return high, middle, low


def flip(index, step, size):
    out, bit = 0, 1
    while bit < size:
        mine = lax.rem(lax.div(index, bit), 2)
        if isinstance(step, int):
            out = out + bit * (1 - mine if (step // bit) % 2 else mine)
        else:
            out = out + bit * lax.rem(mine + lax.rem(lax.div(step, bit), 2), 2)
        bit *= 2
    return out


def step_kernel(
    tiles, depths,
    owner_in, row_in, place_in, scale_in, logit_in, color_in, first_in, second_in,
    target_in, view_in, length_in, cam_in, back_in,
    picture_ref, new_param_ref, new_first_ref, new_second_ref,
    owner_ref, row_ref, place_ref, scale_ref, logit_ref, color_ref, first_ref, second_ref,
    target_ref, view_ref, length_ref, cam_ref, back_ref, loads,
    named_ref, lists_ref, twin_ref, hot_ref, high_names, first_lines, second_lines, twin_sem,
    param_ref, high_ref, low_ref, answers, got,
    ask_send, ask_recv, send, receive,
    alphas, weights, pulls, misses, carries, columns, ordered, entry_ref, basis_ref, miss_ref,
    sums, grad_ref, image_ref, images_ref,
    inbox, partial, pieces, whole_out,
    grad_send, grad_recv, image_send, image_recv, cut_send, cut_recv, pair_sem,
):
    lines = param_ref.shape[0]
    highs = lines // 10
    slabs, _, slab = named_ref.shape
    entries = slabs * slab
    pixels = target_ref.shape[2]
    splats = highs * LANES
    me_t, me_d = lax.axis_index("tile"), lax.axis_index("depth")
    small = tiles <= 8
    depth_of = [me_d] + [flip(me_d, b, depths) for b in range(1, depths)]
    tile_of = [me_t] + [flip(me_t, a, tiles) for a in range(1, tiles)] if small else None
    steps = [(a, b) for a in range(tiles - 1, -1, -1) for b in range(depths) if a or b]

    def tile_at(step):
        return tile_of[step] if small else flip(me_t, step, tiles)

    def to(a, b):
        return {"tile": tile_at(a), "depth": depth_of[b]}

    def across(step):
        return {"tile": tile_at(step)}

    def along(step):
        return {"depth": depth_of[step]}

    def each_tile(function):
        if small:
            for step in range(1, tiles):
                function(step)
        else:
            def one(step, carry):
                function(step)
                return carry

            lax.fori_loop(1, tiles, one, 0)

    barrier = pltpu.get_barrier_semaphore()
    for a, b in steps:
        pl.semaphore_signal(barrier, inc=1, device_id=to(a, b), device_id_type=MESH)
    pairs = [
        (owner_in, owner_ref), (row_in, row_ref), (place_in, place_ref), (scale_in, scale_ref),
        (logit_in, logit_ref), (color_in, color_ref), (view_in, view_ref), (length_in, length_ref),
        (cam_in, cam_ref), (back_in, back_ref), (target_in, target_ref),
        (first_in, first_ref), (second_in, second_ref),
    ]
    copies = [
        pltpu.make_async_copy(source, target, loads.at[i])
        for i, (source, target) in enumerate(pairs)
    ]
    for copy in copies:
        copy.start()
    miss_ref[...] = jnp.zeros(miss_ref.shape, BF16)
    spot = lax.broadcasted_iota(jnp.int32, (1, pixels), 1)
    spot_x = (spot & (TILE_SIDE - 1)).astype(F32) + (0.5 - 0.5 * TILE_SIDE)
    spot_y = (spot >> 5).astype(F32) + (0.5 - 0.5 * (pixels // TILE_SIDE))
    parts = [[jnp.ones((1, pixels), F32)], [spot_x], [spot_y]]
    for square in (spot_x * spot_x, spot_x * spot_y, spot_y * spot_y):
        coarse = square.astype(BF16).astype(F32)
        parts.append([coarse, square - coarse])
    rows = [part for piece in parts for _ in range(3) for part in piece]
    rows.append(jnp.zeros((LANES - len(rows), pixels), F32))
    basis_ref[...] = jnp.concatenate(rows, axis=0).astype(BF16)
    for copy in copies[:2]:
        copy.wait()
    names = jnp.concatenate([owner_ref[q] for q in range(slabs)], axis=0) * splats + row_ref[...]
    quad = lax.broadcasted_iota(jnp.int32, names.shape, 1) >> ((slab // 4).bit_length() - 1)
    names = jnp.where(
        quad == 1, pltpu.roll(names, 3 * slab // 4, 1),
        jnp.where(quad == 2, pltpu.roll(names, slab // 4, 1), names),
    )
    for q in range(slabs):
        named_ref[q] = names[q : q + 1, :]
    pl.semaphore_wait(barrier, len(steps))

    def asked(a, b):
        return remote(
            named_ref.at[depth_of[b]], lists_ref.at[me_t, me_d],
            ask_send.at[a, b], ask_recv.at[a, b], to(a, b),
        )

    for a, b in steps:
        asked(a, b).start()
    lists_ref[me_t, me_d] = named_ref[me_d]
    for copy in copies[2:6]:
        copy.wait()
    param = 0
    for ref in (place_ref, scale_ref, logit_ref, color_ref):
        for k in range(ref.shape[0]):
            for h in range(highs):
                line = param * highs + h
                param_ref[line : line + 1, :] = ref[k : k + 1, h * LANES : (h + 1) * LANES]
            param += 1
    high, middle, low = split3(param_ref[...])
    high_ref[...] = jnp.concatenate([high, middle], axis=1)
    low_ref[...] = low
    low_iota = lax.broadcasted_iota(jnp.int32, (LANES, entries), 0)
    high_iota = lax.broadcasted_iota(jnp.int32, (highs, entries), 0) + me_t * highs
    span = entries // 2
    early = lax.broadcasted_iota(jnp.int32, (1, slab), 1) < slab // 2

    def widen(ref, slot):
        slab_names = [ref[slot, d] for d in range(slabs)]
        turned = [pltpu.roll(x, slab // 2, 1) for x in slab_names]
        return [
            jnp.where(early, slab_names[d], turned[d + 1]) for d in range(0, slabs, 2)
        ] + [
            jnp.where(early, turned[d], slab_names[d + 1]) for d in range(0, slabs, 2)
        ]

    def marks(names):
        onehot = jnp.where(low_iota == (names & (LANES - 1)), 1.0, 0.0).astype(BF16)
        return onehot, high_iota == (names >> 7)

    def note(source, step, names):
        onehot, mask = marks(names)
        for part in range(2):
            cut = slice(part * span, (part + 1) * span)
            hot_ref[source, step, part] = onehot[:, cut]
            high_names[source, step, part] = names[:, cut] >> 7
        return onehot, mask

    def answer(step):
        onehot, mask = note(0, step, jnp.concatenate(widen(lists_ref, tile_at(step)), axis=1))
        twice = jnp.concatenate([onehot, onehot], axis=0)
        found = jnp.dot(high_ref[...], twice, preferred_element_type=F32) + jnp.dot(
            low_ref[...], onehot, preferred_element_type=F32
        )
        return jnp.concatenate(
            [
                jnp.sum(
                    jnp.where(mask, found[p * highs : (p + 1) * highs], 0.0), axis=0, keepdims=True
                )
                for p in range(10)
            ],
            axis=0,
        )

    def put(ref, step, rows):
        for j in range(slabs):
            k = j % (slabs // 2)
            ref[step, j // (slabs // 2), k * 10 : (k + 1) * 10, :] = rows[
                :, j * slab : (j + 1) * slab
            ]

    def back(step, part):
        return remote(
            answers.at[step, part], got.at[step, part], send.at[step, part],
            receive.at[step, part], across(step),
        )

    def serve(*group):
        for step in group:
            for b in range(depths):
                asked(step, b).wait_recv()
        for step in group:
            put(answers, step, answer(step))
        for step in group:
            back(step, 0).start()

    for b in range(1, depths):
        asked(0, b).wait_recv()
    put(got, 0, answer(0))
    if small:
        for step in range(1, tiles, 2):
            serve(*range(step, min(step + 2, tiles)))
    else:
        each_tile(serve)
    if small:
        for step in range(tiles - 1, 0, -1):
            back(step, 1).start()
    else:
        each_tile(lambda step: back(step, 1).start())
    twin = remote(lists_ref, twin_ref, twin_sem.at[0], twin_sem.at[1], along(1))
    twin.start()
    for a, b in steps:
        asked(a, b).wait_send()
    for copy in copies[6:]:
        copy.wait()
    folds = [
        (slice(p, min(p + 8, 10)), slice(h * LANES, (h + 1) * LANES),
         pl.ds(p * highs + h, min(p + 8, 10) - p, stride=highs))
        for h in range(highs)
        for p in (0, 8)
    ]
    for top, part, spaced in folds:
        first_lines[spaced, :] = first_ref[top, part]
        second_lines[spaced, :] = second_ref[top, part]
    twin.wait()

    def note_twin(step):
        note(1, step, jnp.concatenate(widen(twin_ref, tile_at(step)), axis=1))

    note_twin(0)
    each_tile(note_twin)

    chunks = pixels // LANES
    groups = entries // 8
    length = length_ref[me_d]
    view = view_ref[me_d]

    first = [cam_ref[view, 0, j] for j in range(4)]
    second = [cam_ref[view, 1, j] for j in range(4)]
    width = 2 * LANES

    def project(part):
        def take(step):
            back(step, part).wait()
            got[0, part] += got[step, part]

        each_tile(take)
        found = got[0, part]
        values = [
            jnp.concatenate(
                [found[j * 10 + p : j * 10 + p + 1, :] for j in range(slabs // 2)], axis=1
            )
            for p in range(10)
        ]
        variance = [jnp.exp(2.0 * values[3 + j]) for j in range(3)]
        center_x = first[0] * values[0] + first[1] * values[1] + first[2] * values[2] + first[3]
        center_y = second[0] * values[0] + second[1] * values[1] + second[2] * values[2] + second[3]
        cov_xx = sum(first[j] * first[j] * variance[j] for j in range(3)) + 0.3
        cov_xy = sum(first[j] * second[j] * variance[j] for j in range(3))
        cov_yy = sum(second[j] * second[j] * variance[j] for j in range(3)) + 0.3
        determinant = cov_xx * cov_yy - cov_xy * cov_xy
        conic_a = cov_yy / determinant
        conic_b = -cov_xy / determinant
        conic_c = cov_xx / determinant
        fade = 1.0 + jnp.exp(-values[6])
        opacity = 1.0 / fade
        spot = lax.broadcasted_iota(jnp.int32, (1, span), 1)
        stretch = groups // 2
        place = (
            (spot >> (stretch.bit_length() - 1)) * groups + part * stretch + (spot & (stretch - 1))
        )
        slope_x = conic_a * center_x + conic_b * center_y
        slope_y = conic_b * center_x + conic_c * center_y
        level = -0.5 * (slope_x * center_x + slope_y * center_y) - jnp.log(fade)
        terms = [
            jnp.where(place < length, LOG2E * level, -1e30),
            LOG2E * slope_x, LOG2E * slope_y,
            (-0.5 * LOG2E) * conic_a, -LOG2E * conic_b, (-0.5 * LOG2E) * conic_c,
        ]
        rows = []
        for term, copies_of in zip(terms, (1, 1, 1, 2, 2, 2)):
            for piece in split3(term):
                rows += [piece.astype(F32)] * copies_of
        rows += [jnp.zeros((PULL_ROW - len(rows), span), F32)]
        for k in range(3):
            pieces_of = split3(values[7 + k])
            rows += [pieces_of[i].astype(F32) for i, _ in PRODUCTS]
        rows += values[7:10]
        rows += [jnp.zeros((LANES - PULL_ROW - 3 * len(PRODUCTS) - 3, span), F32)]
        base = part * span
        columns[base : base + span, :] = jnp.concatenate(rows, axis=0).T
        for g in range(stretch):
            ordered[base + g * 8 : base + (g + 1) * 8, :] = columns[
                pl.ds(base + g, 8, stride=stretch), :
            ]
        entry_ref[base : base + span, :] = ordered[base : base + span, :].astype(BF16)
        for n in range(pixels // width):
            cut = slice(n * width, (n + 1) * width)
            alphas[base : base + span, cut] = jnp.exp2(
                jnp.dot(
                    entry_ref[base : base + span, :], basis_ref[:, cut], preferred_element_type=F32
                )
            )
        return variance, center_x, center_y, conic_a, conic_b, conic_c, opacity

    lane = lax.broadcasted_iota(jnp.int32, (8, LANES), 1)
    sub = lax.broadcasted_iota(jnp.int32, (8, LANES), 0)
    rows_chunk = LANES // TILE_SIDE
    pixel_x = (lane & (TILE_SIDE - 1)).astype(F32) + (0.5 - 0.5 * TILE_SIDE)
    pixel_y = (lane >> 5).astype(F32) - 0.5 * (rows_chunk - 1)
    ones = jnp.ones((8, LANES), F32)
    tint = PULL_ROW + 3 * len(PRODUCTS)

    def spread(cols, j):
        return jnp.broadcast_to(cols[:, j : j + 1], (8, LANES))

    def forward(g, carry):
        trans, color = carry
        at = pl.ds(pl.multiple_of(g * 8, 8), 8)
        cols = ordered[at, :]
        red, green, blue = [spread(cols, tint + j) for j in range(3)]
        new_trans, new_color = [], []
        for c in range(chunks):
            t = trans[c]
            part = slice(c * LANES, (c + 1) * LANES)
            weight = alphas[at, part] * t
            weights[at, part] = weight
            new_trans.append(t - weight)
            new_color.append(color[3 * c] + weight * red)
            new_color.append(color[3 * c + 1] + weight * green)
            new_color.append(color[3 * c + 2] + weight * blue)
        return new_trans, new_color

    zeros = jnp.zeros((8, LANES), F32)
    carried = ([ones] * chunks, [zeros] * (3 * chunks))
    screens = []
    for part in range(2):
        screens.append(project(part))
        carried = lax.fori_loop(
            part * (groups // 2), (part + 1) * (groups // 2), forward, carried, unroll=AHEAD
        )
    trans, color = carried

    chosen = lax.broadcasted_iota(jnp.int32, (slabs, LANES), 0) == me_d
    behinds = []
    for c in range(chunks):
        part = slice(c * LANES, (c + 1) * LANES)
        run = jnp.where(sub >= 1, pltpu.roll(trans[c], 1, 0), 1.0)
        for s in (1, 2, 4):
            run = run * jnp.where(sub >= s, pltpu.roll(run, s, 0), 1.0)
        carries[:, part] = run
        left = (run * trans[c])[7:8, :]
        pulled = zeros
        last = zeros[0:1]
        for k in range(3):
            shade = jnp.sum(run * color[3 * c + k], axis=0, keepdims=True) + left * back_ref[k]
            image_ref[k : k + 1, part] = shade
            miss = shade - jnp.sum(
                jnp.where(chosen, target_ref[k, :, part], 0.0), axis=0, keepdims=True
            )
            misses[k, :, part] = jnp.broadcast_to(miss, (8, LANES))
            pulled = pulled + miss * color[3 * c + k]
            last = last + miss * back_ref[k]
        kept = trans[c]
        for s in (1, 2, 4):
            inner = sub < 8 - s
            pulled = pulled + kept * jnp.where(inner, pltpu.roll(pulled, 8 - s, 0), 0.0)
            kept = kept * jnp.where(inner, pltpu.roll(kept, 8 - s, 0), 1.0)
        begins = pulled + kept * last
        behinds.append(
            jnp.where(sub < 7, pltpu.roll(begins, 7, 0), jnp.broadcast_to(last, (8, LANES)))
        )
    images_ref[me_d] = image_ref[...]
    image_copies = [
        remote(image_ref, images_ref.at[me_d], image_send.at[s], image_recv.at[s], along(s))
        for s in range(1, depths)
    ]
    for copy in image_copies:
        copy.start()
    rows = []
    for k in range(3):
        pieces_of = split3(misses[k, 0:1, :])
        rows += [pieces_of[j].astype(F32) for _, j in PRODUCTS]
    rows += [jnp.zeros((PULL_ROWS - len(rows), pixels), F32)]
    miss_ref[PULL_ROW : PULL_ROW + PULL_ROWS, :] = jnp.concatenate(rows, axis=0).astype(BF16)
    for n in range(pixels // width):
        part = slice(n * width, (n + 1) * width)
        pulls[:, part] = jnp.dot(entry_ref[...], miss_ref[:, part], preferred_element_type=F32)

    def backward(g, behind, piece):
        at = pl.ds(pl.multiple_of(g * 8, 8), 8)
        new_behind, grad = [], []
        shades = [zeros] * 3
        for c in range(chunks):
            part = slice(c * LANES, (c + 1) * LANES)
            weight = weights[at, part] * carries[:, part]
            gap = pulls[at, part] - behind[c]
            new_behind.append(behind[c] + alphas[at, part] * gap)
            grad.append(weight * gap)
            shades = [shades[k] + weight * misses[k, :, part] for k in range(3)]
        sum_0, sum_1, sum_2 = zeros, zeros, zeros
        for c in range(chunks // 2):
            low, high = grad[c], grad[chunks - 1 - c]
            off = float(rows_chunk) * (0.5 * (chunks - 1) - c)
            even, odd = low + high, high - low
            sum_0 = sum_0 + even
            sum_1 = sum_1 + off * odd
            sum_2 = sum_2 + (off * off) * even
        down = sum_1 + pixel_y * sum_0
        down_2 = sum_2 + pixel_y * (sum_1 + down)
        right = sum_0 * pixel_x
        fields = [sum_0, right, down, right * pixel_x, down * pixel_x, down_2] + shades
        packed = zeros
        for j, field in enumerate(fields):
            packed = jnp.where(lane == j, jnp.sum(field, axis=1, keepdims=True), packed)
        stretch = groups // 2
        sums[pl.ds(piece * (span - stretch) + g, 8, stride=stretch), :] = packed
        return new_behind

    core = lax.rem(me_d, 2)

    def grads(step, other, part):
        return remote(
            grad_ref.at[part, core if not other else 1 - core], inbox.at[step, other, part],
            grad_send.at[step, other, part], grad_recv.at[step, other, part],
            to(step, other),
        )

    ways = [(step, other) for step in range(tiles - 1, -1, -1) for other in (0, 1) if step or other]
    for part in (1, 0):
        top = (part + 1) * (groups // 2)
        behinds = lax.fori_loop(
            0, groups // 2, lambda i, behind: backward(top - 1 - i, behind, part), behinds,
            unroll=BACK,
        )
        variance, center_x, center_y, conic_a, conic_b, conic_c, opacity = screens[part]
        flat = sums[part * span : (part + 1) * span, :].T
        s0, sx, sy, sxx, sxy, syy, d_red, d_green, d_blue = [flat[j : j + 1, :] for j in range(9)]
        sxx = sxx - center_x * sx
        sxy = sxy - center_x * sy
        syy = syy - center_y * sy
        sx = sx - center_x * s0
        sy = sy - center_y * s0
        sxx = sxx - center_x * sx
        sxy = sxy - center_y * sx
        syy = syy - center_y * sy
        d_x = conic_a * sx + conic_b * sy
        d_y = conic_b * sx + conic_c * sy
        d_a, d_b, d_c = -0.5 * sxx, -sxy, -0.5 * syy
        d_xx = -(conic_a * conic_a * d_a + conic_a * conic_b * d_b + conic_b * conic_b * d_c)
        d_yy = -(conic_b * conic_b * d_a + conic_b * conic_c * d_b + conic_c * conic_c * d_c)
        d_xy = -(
            2.0 * conic_a * conic_b * d_a
            + (conic_a * conic_c + conic_b * conic_b) * d_b
            + 2.0 * conic_b * conic_c * d_c
        )
        out = [first[j] * d_x + second[j] * d_y for j in range(3)]
        for j in range(3):
            d_var = first[j] * first[j] * d_xx + first[j] * second[j] * d_xy + second[j] * second[j] * d_yy
            out.append(2.0 * variance[j] * d_var)
        out += [s0 * (1.0 - opacity), d_red, d_green, d_blue]
        out = jnp.concatenate(out, axis=0)
        for u in range(2):
            for j in range(slabs // 2):
                grad_ref[part, u, j * 5 : (j + 1) * 5, :] = out[
                    u * 5 : (u + 1) * 5, j * slab : (j + 1) * slab
                ]
        for step, other in ways:
            grads(step, other, part).start()

    size = lines // 2

    def placed(blocks, step, part):
        dims = (((1,), (1,)), ((), ()))
        total = 0.0
        for source, block in enumerate(blocks):
            wide = jnp.concatenate(
                [block[j * 5 : (j + 1) * 5, :] for j in range(slabs // 2)], axis=1
            )
            mask = high_iota[:, :span] == high_names[source, step, part]
            high = wide.astype(BF16).astype(F32)
            for rows in (high, wide - high):
                spots = jnp.concatenate(
                    [jnp.where(mask, rows[p : p + 1, :], 0.0) for p in range(5)], axis=0
                )
                total = total + lax.dot_general(
                    spots.astype(BF16), hot_ref[source, step, part], dims,
                    preferred_element_type=F32,
                )
        return total

    def gather(part, group):
        for step in group:
            for other in (0, 1) if not isinstance(step, int) or step else (1,):
                grads(step, other, part).wait()
        total = partial[...]
        for step in group:
            near = inbox[step, 0, part] if not isinstance(step, int) or step else grad_ref[part, core]
            total = total + placed([near, inbox[step, 1, part]], step, part)
        partial[...] = total

    partial[...] = jnp.zeros(partial.shape, F32)
    for part in (1, 0):
        if small:
            take_at_once = 4 if part else 2
            for step in range(0, tiles, take_at_once):
                gather(part, range(step, min(step + take_at_once, tiles)))
        else:
            gather(part, [0])
            each_tile(lambda step: gather(part, [step]))

    def side(index):
        return pl.ds(pl.multiple_of(index * size, 8), size)

    mine = side(core)
    cuts = [
        remote(partial, pieces.at[s], cut_send.at[s], cut_recv.at[s], along(s))
        for s in range(2, depths, 2)
    ]
    for copy in cuts:
        copy.start()
    total = partial[...]
    for copy in cuts:
        copy.wait_recv()
    for s in range(2, depths, 2):
        total = total + pieces[s]
    whole_out[mine, :] = total
    share = remote(
        whole_out.at[mine], whole_out.at[mine], pair_sem.at[0], pair_sem.at[1], along(1)
    )
    share.start()

    def finish(rows):
        param_ref[rows, :], first_lines[rows, :], second_lines[rows, :] = adam_update(
            param_ref[rows, :], first_lines[rows, :], second_lines[rows, :], whole_out[rows, :]
        )

    finish(mine)
    for copy in cuts:
        copy.wait_send()
    for copy in image_copies:
        copy.wait()
    for d in range(depths):
        for k in range(3):
            picture_ref[k, d : d + 1, :] = images_ref[d, k : k + 1, :]
    share.wait()
    finish(side(1 - core))
    for top, part, spaced in folds:
        new_param_ref[top, part] = param_ref[spaced, :]
        new_first_ref[top, part] = first_lines[spaced, :]
        new_second_ref[top, part] = second_lines[spaced, :]


def adam_update(param, first, second, gradient):
    new_first = 0.9 * first + 0.1 * gradient
    new_second = 0.999 * second + 0.001 * gradient * gradient
    corrected = new_first / (1.0 - 0.9**10) / (jnp.sqrt(new_second / (1.0 - 0.999**10)) + 1e-08)
    return (param - 0.05 * corrected, new_first, new_second)


def finish_kernel(*refs):
    count = (len(refs) - 1) // 2
    copies = [
        pltpu.make_async_copy(refs[i], refs[count + i], refs[-1].at[i]) for i in range(count)
    ]
    for copy in copies:
        copy.start()
    for copy in copies:
        copy.wait()


def body(
    positions, log_scales, opacity_logits, colors, first_moment, second_moment,
    cameras, background, target, tile_view, tile_length, list_owner, list_row,
):
    tiles_here, _, pixels = target.shape
    slab = list_row.shape[2]
    depths = lax.axis_size("depth")
    tiles = lax.axis_size("tile")
    entries = slab * depths
    splats = positions.shape[1]
    lines = 10 * splats // LANES
    assert tiles_here == depths == 4 and slab == LANES
    assert tiles & (tiles - 1) == 0 and depths & (depths - 1) == 0
    dma = pltpu.SemaphoreType.DMA
    block = (5 * depths, slab)
    slip = (5 * depths // 2, slab)
    limit = 60 << 20
    args = [
        list_owner.reshape(tiles_here, 1, slab), list_row[0],
        positions, log_scales, opacity_logits, colors, first_moment, second_moment,
        target.transpose(1, 0, 2), tile_view, tile_length, cameras, background,
    ]
    held = [
        (pltpu.VMEM if i < 9 else pltpu.SMEM)(arg.shape, arg.dtype) for i, arg in enumerate(args)
    ]
    results = [(3, tiles_here, pixels)] + [(10, splats)] * 3
    done = pl.pallas_call(
        functools.partial(step_kernel, tiles, depths),
        out_shape=[pltpu.VMEM(shape, F32) for shape in results],
        in_specs=[pl.BlockSpec(memory_space=pl.ANY)] * len(args),
        out_specs=[pl.BlockSpec(memory_space=pltpu.VMEM)] * len(results),
        scratch_shapes=held + [
            dma((len(args),)),
            pltpu.VMEM((depths, 1, slab), jnp.int32),
            pltpu.VMEM((tiles, depths, 1, slab), jnp.int32),
            pltpu.VMEM((tiles, depths, 1, slab), jnp.int32),
            pltpu.VMEM((2, tiles, 2, LANES, entries // 2), BF16),
            pltpu.VMEM((2, tiles, 2, 1, entries // 2), jnp.int32),
            pltpu.VMEM((lines, LANES), F32),
            pltpu.VMEM((lines, LANES), F32),
            dma((2,)),
            pltpu.VMEM((lines, LANES), F32),
            pltpu.VMEM((lines, 2 * LANES), BF16),
            pltpu.VMEM((lines, LANES), BF16),
            pltpu.VMEM((tiles, 2) + block, F32),
            pltpu.VMEM((tiles, 2) + block, F32),
            dma((tiles, depths)),
            dma((tiles, depths)),
            dma((tiles, 2)),
            dma((tiles, 2)),
            pltpu.VMEM((entries, pixels), F32),
            pltpu.VMEM((entries, pixels), F32),
            pltpu.VMEM((entries, pixels), F32),
            pltpu.VMEM((3, 8, pixels), F32),
            pltpu.VMEM((8, pixels), F32),
            pltpu.VMEM((entries, LANES), F32),
            pltpu.VMEM((entries, LANES), F32),
            pltpu.VMEM((entries, LANES), BF16),
            pltpu.VMEM((LANES, pixels), BF16),
            pltpu.VMEM((LANES, pixels), BF16),
            pltpu.VMEM((entries, LANES), F32),
            pltpu.VMEM((2, 2) + slip, F32),
            pltpu.VMEM((3, pixels), F32),
            pltpu.VMEM((depths, 3, pixels), F32),
            pltpu.VMEM((tiles, 2, 2) + slip, F32),
            pltpu.VMEM((lines // 2, LANES), F32),
            pltpu.VMEM((depths, lines // 2, LANES), F32),
            pltpu.VMEM((lines, LANES), F32),
            dma((tiles, 2, 2)),
            dma((tiles, 2, 2)),
            dma((depths,)),
            dma((depths,)),
            dma((depths,)),
            dma((depths,)),
            dma((2,)),
        ],
        name="step",
        compiler_params=pltpu.CompilerParams(
            collective_id=1, has_side_effects=True, vmem_limit_bytes=limit
        ),
    )(*args)
    picture, new_params, new_first, new_second = pl.pallas_call(
        finish_kernel,
        out_shape=[jax.ShapeDtypeStruct(shape, F32) for shape in results],
        in_specs=[pl.BlockSpec(memory_space=pltpu.VMEM)] * len(results),
        out_specs=[pl.BlockSpec(memory_space=pl.ANY)] * len(results),
        scratch_shapes=[dma((len(results),))],
        name="finish",
    )(*[pltpu.with_memory_space_constraint(x, pltpu.VMEM) for x in done])
    return (picture.transpose(1, 0, 2), new_params, new_first, new_second)


def solution(mesh):
    placed = (
        P(None, "tile"),
        P(None, "tile"),
        P(None, "tile"),
        P(None, "tile"),
        P(None, "tile"),
        P(None, "tile"),
        P(),
        P(),
        P("tile", None, None),
        P("tile"),
        P("tile"),
        P("depth", "tile", None, None),
        P("depth", "tile", None),
    )
    return jax.shard_map(
        body,
        mesh=mesh,
        in_specs=placed,
        out_specs=(P("tile", None, None), P(None, "tile"), P(None, "tile"), P(None, "tile")),
        check_vma=False,
    )
```

```python
import functools

import jax
import jax.numpy as jnp
from jax import lax
from jax.experimental import pallas as pl
from jax.experimental.pallas import tpu as pltpu
from jax.sharding import PartitionSpec as P

TILE_SIDE = 32
LANES = 128
MESH = pl.DeviceIdType.MESH
F32 = jnp.float32
BF16 = jnp.bfloat16
LOG2E = 1.4426950408889634
PRODUCTS = ((0, 0), (0, 1), (1, 0), (0, 2), (1, 1), (2, 0))
PULL_ROW, PULL_ROWS = 32, 32
AHEAD, BACK = 16, 32


def greet(peers):
    barrier = pltpu.get_barrier_semaphore()
    for peer in peers:
        pl.semaphore_signal(barrier, inc=1, device_id=peer, device_id_type=MESH)
    pl.semaphore_wait(barrier, len(peers))


def remote(source, target, send, receive, peer):
    return pltpu.make_async_remote_copy(
        src_ref=source, dst_ref=target, send_sem=send, recv_sem=receive,
        device_id=peer, device_id_type=MESH,
    )


def split3(x):
    high = x.astype(BF16)
    rest = x - high.astype(F32)
    middle = rest.astype(BF16)
    low = (rest - middle.astype(F32)).astype(BF16)
    return high, middle, low


def flip(index, step, size):
    out, bit = 0, 1
    while bit < size:
        mine = lax.rem(lax.div(index, bit), 2)
        if isinstance(step, int):
            out = out + bit * (1 - mine if (step // bit) % 2 else mine)
        else:
            out = out + bit * lax.rem(mine + lax.rem(lax.div(step, bit), 2), 2)
        bit *= 2
    return out


def step_kernel(
    tiles, depths,
    owner_in, row_in, place_in, scale_in, logit_in, color_in, first_in, second_in,
    target_in, view_in, length_in, cam_in, back_in,
    picture_ref, new_param_ref, new_first_ref, new_second_ref,
    owner_ref, row_ref, place_ref, scale_ref, logit_ref, color_ref, first_ref, second_ref,
    target_ref, view_ref, length_ref, cam_ref, back_ref, loads,
    named_ref, lists_ref, twin_ref, hot_ref, high_names, first_lines, second_lines, twin_sem,
    param_ref, high_ref, low_ref, answers, got,
    ask_send, ask_recv, send, receive,
    alphas, weights, pulls, misses, carries, columns, ordered, entry_ref, basis_ref, miss_ref,
    sums, grad_ref, image_ref, images_ref,
    inbox, partial, pieces, whole_out,
    grad_send, grad_recv, image_send, image_recv, cut_send, cut_recv, pair_sem,
):
    lines = param_ref.shape[0]
    highs = lines // 10
    slabs, _, slab = named_ref.shape
    entries = slabs * slab
    pixels = target_ref.shape[2]
    splats = highs * LANES
    me_t, me_d = lax.axis_index("tile"), lax.axis_index("depth")
    small = tiles <= 8
    depth_of = [me_d] + [flip(me_d, b, depths) for b in range(1, depths)]
    tile_of = [me_t] + [flip(me_t, a, tiles) for a in range(1, tiles)] if small else None
    steps = [(a, b) for a in range(tiles - 1, -1, -1) for b in range(depths) if a or b]

    def tile_at(step):
        return tile_of[step] if small else flip(me_t, step, tiles)

    def to(a, b):
        return {"tile": tile_at(a), "depth": depth_of[b]}

    def across(step):
        return {"tile": tile_at(step)}

    def along(step):
        return {"depth": depth_of[step]}

    def each_tile(function):
        if small:
            for step in range(1, tiles):
                function(step)
        else:
            def one(step, carry):
                function(step)
                return carry

            lax.fori_loop(1, tiles, one, 0)

    barrier = pltpu.get_barrier_semaphore()
    pairs = [
        (owner_in, owner_ref), (row_in, row_ref), (place_in, place_ref), (scale_in, scale_ref),
        (logit_in, logit_ref), (color_in, color_ref), (view_in, view_ref), (length_in, length_ref),
        (cam_in, cam_ref), (back_in, back_ref), (target_in, target_ref),
        (first_in, first_ref), (second_in, second_ref),
    ]
    copies = [
        pltpu.make_async_copy(source, target, loads.at[i])
        for i, (source, target) in enumerate(pairs)
    ]
    for copy in copies[:2]:
        copy.start()
    for a, b in steps:
        pl.semaphore_signal(barrier, inc=1, device_id=to(a, b), device_id_type=MESH)
    for copy in copies[2:]:
        copy.start()
    miss_ref[...] = jnp.zeros(miss_ref.shape, BF16)
    spot = lax.broadcasted_iota(jnp.int32, (1, pixels), 1)
    spot_x = (spot & (TILE_SIDE - 1)).astype(F32) + (0.5 - 0.5 * TILE_SIDE)
    spot_y = (spot >> 5).astype(F32) + (0.5 - 0.5 * (pixels // TILE_SIDE))
    parts = [[jnp.ones((1, pixels), F32)], [spot_x], [spot_y]]
    for square in (spot_x * spot_x, spot_x * spot_y, spot_y * spot_y):
        coarse = square.astype(BF16).astype(F32)
        parts.append([coarse, square - coarse])
    rows = [part for piece in parts for _ in range(3) for part in piece]
    rows.append(jnp.zeros((LANES - len(rows), pixels), F32))
    basis_ref[...] = jnp.concatenate(rows, axis=0).astype(BF16)
    for copy in copies[:2]:
        copy.wait()
    names = jnp.concatenate([owner_ref[q] for q in range(slabs)], axis=0) * splats + row_ref[...]
    quad = lax.broadcasted_iota(jnp.int32, names.shape, 1) >> ((slab // 4).bit_length() - 1)
    names = jnp.where(
        quad == 1, pltpu.roll(names, 3 * slab // 4, 1),
        jnp.where(quad == 2, pltpu.roll(names, slab // 4, 1), names),
    )
    for q in range(slabs):
        named_ref[q] = names[q : q + 1, :]
    pl.semaphore_wait(barrier, len(steps))

    def asked(a, b):
        return remote(
            named_ref.at[depth_of[b]], lists_ref.at[me_t, me_d],
            ask_send.at[a, b], ask_recv.at[a, b], to(a, b),
        )

    for a, b in steps:
        asked(a, b).start()
    lists_ref[me_t, me_d] = named_ref[me_d]
    for copy in copies[2:6]:
        copy.wait()
    param = 0
    for ref in (place_ref, scale_ref, logit_ref, color_ref):
        for k in range(ref.shape[0]):
            for h in range(highs):
                line = param * highs + h
                param_ref[line : line + 1, :] = ref[k : k + 1, h * LANES : (h + 1) * LANES]
            param += 1
    high, middle, low = split3(param_ref[...])
    high_ref[...] = jnp.concatenate([high, middle], axis=1)
    low_ref[...] = low
    low_iota = lax.broadcasted_iota(jnp.int32, (LANES, entries), 0)
    high_iota = lax.broadcasted_iota(jnp.int32, (highs, entries), 0) + me_t * highs
    span = entries // 2
    early = lax.broadcasted_iota(jnp.int32, (1, slab), 1) < slab // 2

    def widen(ref, slot):
        slab_names = [ref[slot, d] for d in range(slabs)]
        turned = [pltpu.roll(x, slab // 2, 1) for x in slab_names]
        return [
            jnp.where(early, slab_names[d], turned[d + 1]) for d in range(0, slabs, 2)
        ] + [
            jnp.where(early, turned[d], slab_names[d + 1]) for d in range(0, slabs, 2)
        ]

    def marks(names):
        onehot = jnp.where(low_iota == (names & (LANES - 1)), 1.0, 0.0).astype(BF16)
        return onehot, high_iota == (names >> 7)

    def note(source, step, names):
        onehot, mask = marks(names)
        for part in range(2):
            cut = slice(part * span, (part + 1) * span)
            hot_ref[source, step, part] = onehot[:, cut]
            high_names[source, step, part] = names[:, cut] >> 7
        return onehot, mask

    def answer(step):
        onehot, mask = note(0, step, jnp.concatenate(widen(lists_ref, tile_at(step)), axis=1))
        twice = jnp.concatenate([onehot, onehot], axis=0)
        found = jnp.dot(high_ref[...], twice, preferred_element_type=F32) + jnp.dot(
            low_ref[...], onehot, preferred_element_type=F32
        )
        return jnp.concatenate(
            [
                jnp.sum(
                    jnp.where(mask, found[p * highs : (p + 1) * highs], 0.0), axis=0, keepdims=True
                )
                for p in range(10)
            ],
            axis=0,
        )

    def put(ref, step, rows):
        for j in range(slabs):
            k = j % (slabs // 2)
            ref[step, j // (slabs // 2), k * 10 : (k + 1) * 10, :] = rows[
                :, j * slab : (j + 1) * slab
            ]

    def back(step, part):
        return remote(
            answers.at[step, part], got.at[step, part], send.at[step, part],
            receive.at[step, part], across(step),
        )

    def serve(*group):
        for step in group:
            for b in range(depths):
                asked(step, b).wait_recv()
        for step in group:
            put(answers, step, answer(step))
        for step in group:
            back(step, 0).start()

    for b in range(1, depths):
        asked(0, b).wait_recv()
    put(got, 0, answer(0))
    if small:
        for step in range(1, tiles, 2):
            serve(*range(step, min(step + 2, tiles)))
    else:
        each_tile(serve)
    if small:
        for step in range(tiles - 1, 0, -1):
            back(step, 1).start()
    else:
        each_tile(lambda step: back(step, 1).start())
    twin = remote(lists_ref, twin_ref, twin_sem.at[0], twin_sem.at[1], along(1))
    twin.start()
    for a, b in steps:
        asked(a, b).wait_send()
    for copy in copies[6:]:
        copy.wait()
    folds = [
        (slice(p, min(p + 8, 10)), slice(h * LANES, (h + 1) * LANES),
         pl.ds(p * highs + h, min(p + 8, 10) - p, stride=highs))
        for h in range(highs)
        for p in (0, 8)
    ]
    for top, part, spaced in folds:
        first_lines[spaced, :] = first_ref[top, part]
        second_lines[spaced, :] = second_ref[top, part]
    twin.wait()

    def note_twin(step):
        note(1, step, jnp.concatenate(widen(twin_ref, tile_at(step)), axis=1))

    note_twin(0)
    each_tile(note_twin)

    chunks = pixels // LANES
    groups = entries // 8
    length = length_ref[me_d]
    view = view_ref[me_d]

    first = [cam_ref[view, 0, j] for j in range(4)]
    second = [cam_ref[view, 1, j] for j in range(4)]
    width = 2 * LANES

    def project(part):
        def take(step):
            back(step, part).wait()
            got[0, part] += got[step, part]

        each_tile(take)
        found = got[0, part]
        values = [
            jnp.concatenate(
                [found[j * 10 + p : j * 10 + p + 1, :] for j in range(slabs // 2)], axis=1
            )
            for p in range(10)
        ]
        variance = [jnp.exp(2.0 * values[3 + j]) for j in range(3)]
        center_x = first[0] * values[0] + first[1] * values[1] + first[2] * values[2] + first[3]
        center_y = second[0] * values[0] + second[1] * values[1] + second[2] * values[2] + second[3]
        cov_xx = sum(first[j] * first[j] * variance[j] for j in range(3)) + 0.3
        cov_xy = sum(first[j] * second[j] * variance[j] for j in range(3))
        cov_yy = sum(second[j] * second[j] * variance[j] for j in range(3)) + 0.3
        determinant = cov_xx * cov_yy - cov_xy * cov_xy
        conic_a = cov_yy / determinant
        conic_b = -cov_xy / determinant
        conic_c = cov_xx / determinant
        fade = 1.0 + jnp.exp(-values[6])
        opacity = 1.0 / fade
        spot = lax.broadcasted_iota(jnp.int32, (1, span), 1)
        stretch = groups // 2
        place = (
            (spot >> (stretch.bit_length() - 1)) * groups + part * stretch + (spot & (stretch - 1))
        )
        slope_x = conic_a * center_x + conic_b * center_y
        slope_y = conic_b * center_x + conic_c * center_y
        level = -0.5 * (slope_x * center_x + slope_y * center_y) - jnp.log(fade)
        terms = [
            jnp.where(place < length, LOG2E * level, -1e30),
            LOG2E * slope_x, LOG2E * slope_y,
            (-0.5 * LOG2E) * conic_a, -LOG2E * conic_b, (-0.5 * LOG2E) * conic_c,
        ]
        rows = []
        for term, copies_of in zip(terms, (1, 1, 1, 2, 2, 2)):
            for piece in split3(term):
                rows += [piece.astype(F32)] * copies_of
        rows += [jnp.zeros((PULL_ROW - len(rows), span), F32)]
        for k in range(3):
            pieces_of = split3(values[7 + k])
            rows += [pieces_of[i].astype(F32) for i, _ in PRODUCTS]
        rows += values[7:10]
        rows += [jnp.zeros((LANES - PULL_ROW - 3 * len(PRODUCTS) - 3, span), F32)]
        base = part * span
        columns[base : base + span, :] = jnp.concatenate(rows, axis=0).T
        for g in range(stretch):
            ordered[base + g * 8 : base + (g + 1) * 8, :] = columns[
                pl.ds(base + g, 8, stride=stretch), :
            ]
        entry_ref[base : base + span, :] = ordered[base : base + span, :].astype(BF16)
        for n in range(pixels // width):
            cut = slice(n * width, (n + 1) * width)
            alphas[base : base + span, cut] = jnp.exp2(
                jnp.dot(
                    entry_ref[base : base + span, :], basis_ref[:, cut], preferred_element_type=F32
                )
            )
        return variance, center_x, center_y, conic_a, conic_b, conic_c, opacity

    lane = lax.broadcasted_iota(jnp.int32, (8, LANES), 1)
    sub = lax.broadcasted_iota(jnp.int32, (8, LANES), 0)
    rows_chunk = LANES // TILE_SIDE
    pixel_x = (lane & (TILE_SIDE - 1)).astype(F32) + (0.5 - 0.5 * TILE_SIDE)
    pixel_y = (lane >> 5).astype(F32) - 0.5 * (rows_chunk - 1)
    ones = jnp.ones((8, LANES), F32)
    tint = PULL_ROW + 3 * len(PRODUCTS)

    def spread(cols, j):
        return jnp.broadcast_to(cols[:, j : j + 1], (8, LANES))

    def forward(g, carry):
        trans, color = carry
        at = pl.ds(pl.multiple_of(g * 8, 8), 8)
        cols = ordered[at, :]
        red, green, blue = [spread(cols, tint + j) for j in range(3)]
        new_trans, new_color = [], []
        for c in range(chunks):
            t = trans[c]
            part = slice(c * LANES, (c + 1) * LANES)
            weight = alphas[at, part] * t
            weights[at, part] = weight
            new_trans.append(t - weight)
            new_color.append(color[3 * c] + weight * red)
            new_color.append(color[3 * c + 1] + weight * green)
            new_color.append(color[3 * c + 2] + weight * blue)
        return new_trans, new_color

    zeros = jnp.zeros((8, LANES), F32)
    carried = ([ones] * chunks, [zeros] * (3 * chunks))
    screens = []
    for part in range(2):
        screens.append(project(part))
        carried = lax.fori_loop(
            part * (groups // 2), (part + 1) * (groups // 2), forward, carried, unroll=AHEAD
        )
    trans, color = carried

    chosen = lax.broadcasted_iota(jnp.int32, (slabs, LANES), 0) == me_d
    behinds = []
    for c in range(chunks):
        part = slice(c * LANES, (c + 1) * LANES)
        run = jnp.where(sub >= 1, pltpu.roll(trans[c], 1, 0), 1.0)
        for s in (1, 2, 4):
            run = run * jnp.where(sub >= s, pltpu.roll(run, s, 0), 1.0)
        carries[:, part] = run
        left = (run * trans[c])[7:8, :]
        pulled = zeros
        last = zeros[0:1]
        for k in range(3):
            shade = jnp.sum(run * color[3 * c + k], axis=0, keepdims=True) + left * back_ref[k]
            image_ref[k : k + 1, part] = shade
            miss = shade - jnp.sum(
                jnp.where(chosen, target_ref[k, :, part], 0.0), axis=0, keepdims=True
            )
            misses[k, :, part] = jnp.broadcast_to(miss, (8, LANES))
            pulled = pulled + miss * color[3 * c + k]
            last = last + miss * back_ref[k]
        kept = trans[c]
        for s in (1, 2, 4):
            inner = sub < 8 - s
            pulled = pulled + kept * jnp.where(inner, pltpu.roll(pulled, 8 - s, 0), 0.0)
            kept = kept * jnp.where(inner, pltpu.roll(kept, 8 - s, 0), 1.0)
        begins = pulled + kept * last
        behinds.append(
            jnp.where(sub < 7, pltpu.roll(begins, 7, 0), jnp.broadcast_to(last, (8, LANES)))
        )
    images_ref[me_d] = image_ref[...]
    image_copies = [
        remote(image_ref, images_ref.at[me_d], image_send.at[s], image_recv.at[s], along(s))
        for s in range(1, depths)
    ]
    for copy in image_copies:
        copy.start()
    rows = []
    for k in range(3):
        pieces_of = split3(misses[k, 0:1, :])
        rows += [pieces_of[j].astype(F32) for _, j in PRODUCTS]
    rows += [jnp.zeros((PULL_ROWS - len(rows), pixels), F32)]
    miss_ref[PULL_ROW : PULL_ROW + PULL_ROWS, :] = jnp.concatenate(rows, axis=0).astype(BF16)
    for n in range(pixels // width):
        part = slice(n * width, (n + 1) * width)
        pulls[:, part] = jnp.dot(entry_ref[...], miss_ref[:, part], preferred_element_type=F32)

    def backward(g, behind, piece):
        at = pl.ds(pl.multiple_of(g * 8, 8), 8)
        new_behind, grad = [], []
        shades = [zeros] * 3
        for c in range(chunks):
            part = slice(c * LANES, (c + 1) * LANES)
            weight = weights[at, part] * carries[:, part]
            gap = pulls[at, part] - behind[c]
            new_behind.append(behind[c] + alphas[at, part] * gap)
            grad.append(weight * gap)
            shades = [shades[k] + weight * misses[k, :, part] for k in range(3)]
        sum_0, sum_1, sum_2 = zeros, zeros, zeros
        for c in range(chunks // 2):
            low, high = grad[c], grad[chunks - 1 - c]
            off = float(rows_chunk) * (0.5 * (chunks - 1) - c)
            even, odd = low + high, high - low
            sum_0 = sum_0 + even
            sum_1 = sum_1 + off * odd
            sum_2 = sum_2 + (off * off) * even
        down = sum_1 + pixel_y * sum_0
        down_2 = sum_2 + pixel_y * (sum_1 + down)
        right = sum_0 * pixel_x
        fields = [sum_0, right, down, right * pixel_x, down * pixel_x, down_2] + shades
        packed = zeros
        for j, field in enumerate(fields):
            packed = jnp.where(lane == j, jnp.sum(field, axis=1, keepdims=True), packed)
        stretch = groups // 2
        sums[pl.ds(piece * (span - stretch) + g, 8, stride=stretch), :] = packed
        return new_behind

    core = lax.rem(me_d, 2)

    def grads(step, other, part):
        return remote(
            grad_ref.at[part, core if not other else 1 - core], inbox.at[step, other, part],
            grad_send.at[step, other, part], grad_recv.at[step, other, part],
            to(step, other),
        )

    ways = [(step, other) for step in range(tiles - 1, -1, -1) for other in (0, 1) if step or other]
    for part in (1, 0):
        top = (part + 1) * (groups // 2)
        behinds = lax.fori_loop(
            0, groups // 2, lambda i, behind: backward(top - 1 - i, behind, part), behinds,
            unroll=BACK,
        )
        variance, center_x, center_y, conic_a, conic_b, conic_c, opacity = screens[part]
        flat = sums[part * span : (part + 1) * span, :].T
        s0, sx, sy, sxx, sxy, syy, d_red, d_green, d_blue = [flat[j : j + 1, :] for j in range(9)]
        sxx = sxx - center_x * sx
        sxy = sxy - center_x * sy
        syy = syy - center_y * sy
        sx = sx - center_x * s0
        sy = sy - center_y * s0
        sxx = sxx - center_x * sx
        sxy = sxy - center_y * sx
        syy = syy - center_y * sy
        d_x = conic_a * sx + conic_b * sy
        d_y = conic_b * sx + conic_c * sy
        d_a, d_b, d_c = -0.5 * sxx, -sxy, -0.5 * syy
        d_xx = -(conic_a * conic_a * d_a + conic_a * conic_b * d_b + conic_b * conic_b * d_c)
        d_yy = -(conic_b * conic_b * d_a + conic_b * conic_c * d_b + conic_c * conic_c * d_c)
        d_xy = -(
            2.0 * conic_a * conic_b * d_a
            + (conic_a * conic_c + conic_b * conic_b) * d_b
            + 2.0 * conic_b * conic_c * d_c
        )
        out = [first[j] * d_x + second[j] * d_y for j in range(3)]
        for j in range(3):
            d_var = first[j] * first[j] * d_xx + first[j] * second[j] * d_xy + second[j] * second[j] * d_yy
            out.append(2.0 * variance[j] * d_var)
        out += [s0 * (1.0 - opacity), d_red, d_green, d_blue]
        out = jnp.concatenate(out, axis=0)
        for u in range(2):
            for j in range(slabs // 2):
                grad_ref[part, u, j * 5 : (j + 1) * 5, :] = out[
                    u * 5 : (u + 1) * 5, j * slab : (j + 1) * slab
                ]
        for step, other in ways:
            grads(step, other, part).start()

    size = lines // 2

    def placed(blocks, step, part):
        dims = (((1,), (1,)), ((), ()))
        total = 0.0
        for source, block in enumerate(blocks):
            wide = jnp.concatenate(
                [block[j * 5 : (j + 1) * 5, :] for j in range(slabs // 2)], axis=1
            )
            mask = high_iota[:, :span] == high_names[source, step, part]
            high = wide.astype(BF16).astype(F32)
            for rows in (high, wide - high):
                spots = jnp.concatenate(
                    [jnp.where(mask, rows[p : p + 1, :], 0.0) for p in range(5)], axis=0
                )
                total = total + lax.dot_general(
                    spots.astype(BF16), hot_ref[source, step, part], dims,
                    preferred_element_type=F32,
                )
        return total

    def gather(part, group):
        for step in group:
            for other in (0, 1) if not isinstance(step, int) or step else (1,):
                grads(step, other, part).wait()
        total = partial[...]
        for step in group:
            near = inbox[step, 0, part] if not isinstance(step, int) or step else grad_ref[part, core]
            total = total + placed([near, inbox[step, 1, part]], step, part)
        partial[...] = total

    partial[...] = jnp.zeros(partial.shape, F32)
    for part in (1, 0):
        if small:
            take_at_once = 4 if part else 2
            for step in range(0, tiles, take_at_once):
                gather(part, range(step, min(step + take_at_once, tiles)))
        else:
            gather(part, [0])
            each_tile(lambda step: gather(part, [step]))

    def side(index):
        return pl.ds(pl.multiple_of(index * size, 8), size)

    mine = side(core)
    cuts = [
        remote(partial, pieces.at[s], cut_send.at[s], cut_recv.at[s], along(s))
        for s in range(2, depths, 2)
    ]
    for copy in cuts:
        copy.start()
    total = partial[...]
    for copy in cuts:
        copy.wait_recv()
    for s in range(2, depths, 2):
        total = total + pieces[s]
    whole_out[mine, :] = total
    share = remote(
        whole_out.at[mine], whole_out.at[mine], pair_sem.at[0], pair_sem.at[1], along(1)
    )
    share.start()

    def finish(rows):
        param_ref[rows, :], first_lines[rows, :], second_lines[rows, :] = adam_update(
            param_ref[rows, :], first_lines[rows, :], second_lines[rows, :], whole_out[rows, :]
        )

    finish(mine)
    for copy in cuts:
        copy.wait_send()
    for copy in image_copies:
        copy.wait()
    for d in range(depths):
        for k in range(3):
            picture_ref[k, d : d + 1, :] = images_ref[d, k : k + 1, :]
    share.wait()
    finish(side(1 - core))
    for top, part, spaced in folds:
        new_param_ref[top, part] = param_ref[spaced, :]
        new_first_ref[top, part] = first_lines[spaced, :]
        new_second_ref[top, part] = second_lines[spaced, :]


def adam_update(param, first, second, gradient):
    new_first = 0.9 * first + 0.1 * gradient
    new_second = 0.999 * second + 0.001 * gradient * gradient
    corrected = new_first / (1.0 - 0.9**10) / (jnp.sqrt(new_second / (1.0 - 0.999**10)) + 1e-08)
    return (param - 0.05 * corrected, new_first, new_second)


def finish_kernel(*refs):
    count = (len(refs) - 1) // 2
    copies = [
        pltpu.make_async_copy(refs[i], refs[count + i], refs[-1].at[i]) for i in range(count)
    ]
    for copy in copies:
        copy.start()
    for copy in copies:
        copy.wait()


def body(
    positions, log_scales, opacity_logits, colors, first_moment, second_moment,
    cameras, background, target, tile_view, tile_length, list_owner, list_row,
):
    tiles_here, _, pixels = target.shape
    slab = list_row.shape[2]
    depths = lax.axis_size("depth")
    tiles = lax.axis_size("tile")
    entries = slab * depths
    splats = positions.shape[1]
    lines = 10 * splats // LANES
    assert tiles_here == depths == 4 and slab == LANES
    assert tiles & (tiles - 1) == 0 and depths & (depths - 1) == 0
    dma = pltpu.SemaphoreType.DMA
    block = (5 * depths, slab)
    slip = (5 * depths // 2, slab)
    limit = 60 << 20
    args = [
        list_owner.reshape(tiles_here, 1, slab), list_row[0],
        positions, log_scales, opacity_logits, colors, first_moment, second_moment,
        target.transpose(1, 0, 2), tile_view, tile_length, cameras, background,
    ]
    held = [
        (pltpu.VMEM if i < 9 else pltpu.SMEM)(arg.shape, arg.dtype) for i, arg in enumerate(args)
    ]
    results = [(3, tiles_here, pixels)] + [(10, splats)] * 3
    done = pl.pallas_call(
        functools.partial(step_kernel, tiles, depths),
        out_shape=[pltpu.VMEM(shape, F32) for shape in results],
        in_specs=[pl.BlockSpec(memory_space=pl.ANY)] * len(args),
        out_specs=[pl.BlockSpec(memory_space=pltpu.VMEM)] * len(results),
        scratch_shapes=held + [
            dma((len(args),)),
            pltpu.VMEM((depths, 1, slab), jnp.int32),
            pltpu.VMEM((tiles, depths, 1, slab), jnp.int32),
            pltpu.VMEM((tiles, depths, 1, slab), jnp.int32),
            pltpu.VMEM((2, tiles, 2, LANES, entries // 2), BF16),
            pltpu.VMEM((2, tiles, 2, 1, entries // 2), jnp.int32),
            pltpu.VMEM((lines, LANES), F32),
            pltpu.VMEM((lines, LANES), F32),
            dma((2,)),
            pltpu.VMEM((lines, LANES), F32),
            pltpu.VMEM((lines, 2 * LANES), BF16),
            pltpu.VMEM((lines, LANES), BF16),
            pltpu.VMEM((tiles, 2) + block, F32),
            pltpu.VMEM((tiles, 2) + block, F32),
            dma((tiles, depths)),
            dma((tiles, depths)),
            dma((tiles, 2)),
            dma((tiles, 2)),
            pltpu.VMEM((entries, pixels), F32),
            pltpu.VMEM((entries, pixels), F32),
            pltpu.VMEM((entries, pixels), F32),
            pltpu.VMEM((3, 8, pixels), F32),
            pltpu.VMEM((8, pixels), F32),
            pltpu.VMEM((entries, LANES), F32),
            pltpu.VMEM((entries, LANES), F32),
            pltpu.VMEM((entries, LANES), BF16),
            pltpu.VMEM((LANES, pixels), BF16),
            pltpu.VMEM((LANES, pixels), BF16),
            pltpu.VMEM((entries, LANES), F32),
            pltpu.VMEM((2, 2) + slip, F32),
            pltpu.VMEM((3, pixels), F32),
            pltpu.VMEM((depths, 3, pixels), F32),
            pltpu.VMEM((tiles, 2, 2) + slip, F32),
            pltpu.VMEM((lines // 2, LANES), F32),
            pltpu.VMEM((depths, lines // 2, LANES), F32),
            pltpu.VMEM((lines, LANES), F32),
            dma((tiles, 2, 2)),
            dma((tiles, 2, 2)),
            dma((depths,)),
            dma((depths,)),
            dma((depths,)),
            dma((depths,)),
            dma((2,)),
        ],
        name="step",
        compiler_params=pltpu.CompilerParams(
            collective_id=1, has_side_effects=True, vmem_limit_bytes=limit
        ),
    )(*args)
    picture, new_params, new_first, new_second = pl.pallas_call(
        finish_kernel,
        out_shape=[jax.ShapeDtypeStruct(shape, F32) for shape in results],
        in_specs=[pl.BlockSpec(memory_space=pltpu.VMEM)] * len(results),
        out_specs=[pl.BlockSpec(memory_space=pl.ANY)] * len(results),
        scratch_shapes=[dma((len(results),))],
        name="finish",
    )(*[pltpu.with_memory_space_constraint(x, pltpu.VMEM) for x in done])
    return (picture.transpose(1, 0, 2), new_params, new_first, new_second)


def solution(mesh):
    placed = (
        P(None, "tile"),
        P(None, "tile"),
        P(None, "tile"),
        P(None, "tile"),
        P(None, "tile"),
        P(None, "tile"),
        P(),
        P(),
        P("tile", None, None),
        P("tile"),
        P("tile"),
        P("depth", "tile", None, None),
        P("depth", "tile", None),
    )
    return jax.shard_map(
        body,
        mesh=mesh,
        in_specs=placed,
        out_specs=(P("tile", None, None), P(None, "tile"), P(None, "tile"), P(None, "tile")),
        check_vma=False,
    )
```
